32 devices in a mesh: lat: 4 (over z), lon: 8 (over y, x, core).
Axes of the slice: x: 2, y: 2, z: 4, core: 2. Of those that a mesh axis runs over, the one named last changes fastest.
Arguments:
- poleward_flow: float32 [10, 4, 256, 1024], P(None, None, 'lat', 'lon'), may hold values from -16 to 16
- potential_warmth: float32 [10, 4, 256, 1024], P(None, None, 'lat', 'lon'), may hold values from -16 to 16
- water_profile_flag: int32 [256, 1024], P('lat', 'lon'), may hold values from 0 to 1
- floor_count: int32 [256, 1024], P('lat', 'lon'), may hold values from 0 to 4, as said below
- catchment_label_for_site: int32 [256, 1024], P('lat', 'lon'), may hold values from 0 to 9
Outputs:
- eddy_temp: float32 [4, 256, 1024], P(None, 'lat', 'lon')
- transport: float32 [4, 10, 4, 256], P(None, None, None, ('lat', 'lon'))
The draws below stay inside these ranges and needn't reach their ends.
Inputs may be any that keep to these rules, and one draw needn't show every extreme that they name: `floor_count`: land rows of zeros occur at some latitudes; elsewhere columns have 1 to 4 wet levels.
All inputs are finite; a program needn't handle non-finite values.
Results may differ from the reference program's by a relative error of at most 0.0003.
Values sent between devices are 32-bit elements; how exact they have to be, the bound alone decides.
No kernel may reach another device: no remote copies, remote signals or barrier semaphores. Data moves between devices by JAX's collectives and lax.ppermute only.
A program may use at most 64 MiB of HBM per device.

```python
import math
import jax
import jax.numpy as jnp
from jax import lax

SNAPSHOT_TIMES = 10
LAYERS = 4
BASINS = 10
MERIDIAN_POINTS = 256
LONGITUDE_SLOTS = 1024


def ocean_fields(key):
    generator_keys = jax.random.split(jax.random.fold_in(key, 11), 10)
    along_latitude_flow = jax.random.normal(generator_keys[0], (1, LAYERS, MERIDIAN_POINTS, 1), jnp.float32)
    along_latitude_warmth = jax.random.normal(generator_keys[1], (1, LAYERS, MERIDIAN_POINTS, 1), jnp.float32)
    residual_transport_term = jax.random.normal(generator_keys[2], (SNAPSHOT_TIMES, LAYERS, MERIDIAN_POINTS, 1), jnp.float32)
    thermal_deviate = 0.6 * residual_transport_term + 0.8 * jax.random.normal(generator_keys[3], (SNAPSHOT_TIMES, LAYERS, MERIDIAN_POINTS, 1), jnp.float32)
    steady_share = jax.random.normal(generator_keys[4], (1, LAYERS, MERIDIAN_POINTS, LONGITUDE_SLOTS), jnp.float32)
    steady_warmth = jax.random.normal(generator_keys[5], (1, LAYERS, MERIDIAN_POINTS, LONGITUDE_SLOTS), jnp.float32)
    speed_residual = jax.random.normal(generator_keys[6], (SNAPSHOT_TIMES, LAYERS, MERIDIAN_POINTS, LONGITUDE_SLOTS), jnp.float32)
    thermal_residual = jax.random.normal(generator_keys[7], (SNAPSHOT_TIMES, LAYERS, MERIDIAN_POINTS, LONGITUDE_SLOTS), jnp.float32)
    steady_factor = jax.random.uniform(generator_keys[8], (1, LAYERS, MERIDIAN_POINTS, 1), jnp.float32, -1.0, 1.0)
    fluctuating_factor = jax.random.uniform(generator_keys[9], (1, LAYERS, MERIDIAN_POINTS, 1), jnp.float32, 0.2, 1.0)
    poleward_flow = 0.5 * along_latitude_flow + 0.3 * residual_transport_term + 0.7 * steady_share + speed_residual
    potential_warmth = along_latitude_warmth + 0.3 * thermal_deviate + steady_factor * steady_share + 0.5 * steady_warmth + fluctuating_factor * speed_residual + 0.6 * thermal_residual
    return (jnp.clip(poleward_flow, -16.0, 16.0), jnp.clip(potential_warmth, -16.0, 16.0))


def draw_poleward_flow(key, part):
    return ocean_fields(key)[0]


def draw_potential_warmth(key, part):
    return ocean_fields(key)[1]


def draw_water_profile_flag(key, part):
    columns = jnp.arange(LONGITUDE_SLOTS, dtype=jnp.int32)
    threshold = 25 + 65 * columns // LONGITUDE_SLOTS
    dice = jax.random.randint(jax.random.fold_in(key, 21), (MERIDIAN_POINTS, LONGITUDE_SLOTS), 0, 100)
    return (dice < threshold[None, :]).astype(jnp.int32)


def draw_floor_count(key, part):
    wet_levels = jax.random.randint(jax.random.fold_in(key, 31), (MERIDIAN_POINTS, LONGITUDE_SLOTS), 1, LAYERS + 1)
    land_rows = jax.random.randint(jax.random.fold_in(key, 32), (MERIDIAN_POINTS, 1), 0, 16) == 0
    return jnp.where(land_rows, 0, wet_levels).astype(jnp.int32)


def touch_ends(entries, own_key, low, top_value):
    dims = entries.shape
    index_at = [jax.random.randint(jax.random.fold_in(own_key, axis), (), 0, dims[axis]) for axis in range(len(dims))]
    entries = entries.at[tuple(index_at)].set(low)
    longest = dims.index(max(dims))
    index_at[longest] = (index_at[longest] + 1) % dims[longest]
    return entries.at[tuple(index_at)].set(top_value)


def setup_inputs(seed: int = 0) -> dict:
    key_of = jax.random.split(jax.random.key(seed), 6)
    return {
        "poleward_flow": draw_poleward_flow(jax.random.fold_in(key_of[5], 71), 0),
        "potential_warmth": draw_potential_warmth(jax.random.fold_in(key_of[5], 71), 0),
        "water_profile_flag": draw_water_profile_flag(jax.random.fold_in(key_of[5], 71), 0),
        "floor_count": draw_floor_count(jax.random.fold_in(key_of[5], 71), 0),
        "catchment_label_for_site": touch_ends(jax.random.randint(key_of[4], (MERIDIAN_POINTS, LONGITUDE_SLOTS), 0, BASINS), jax.random.fold_in(key_of[4], 1), 0, BASINS - 1).astype(jnp.int32),
    }


highest_accuracy = lax.Precision.HIGHEST

def layer_summands(layer_position, meridional_speed_layer, thermal_layer_slice, bottom_layer_limit, catchment_label_for_site):
    topmost_warmth = jnp.concatenate([thermal_layer_slice[:, 1:, :], jnp.zeros_like(thermal_layer_slice[:, :1, :])], axis=1)
    warmth_entry = 0.5 * (thermal_layer_slice + topmost_warmth)
    upper_depth = jnp.concatenate([bottom_layer_limit[1:], jnp.zeros_like(bottom_layer_limit[:1])], axis=0)
    level_value = layer_position.astype(jnp.float32)
    wet_cells = ((level_value < bottom_layer_limit) & (level_value < upper_depth)).astype(jnp.float32)
    basin_ids = jnp.arange(BASINS, dtype=jnp.int32)
    one_hot = (catchment_label_for_site[None] == basin_ids[:, None, None]).astype(jnp.float32)
    scaling_factors = one_hot * wet_cells[None]
    watered_total = lax.optimization_barrier(jnp.sum(scaling_factors, axis=2))
    along_latitude_flow = jnp.einsum('qfd,zfd->zqf', scaling_factors, meridional_speed_layer, precision=highest_accuracy)
    along_latitude_warmth = jnp.einsum('qfd,zfd->zqf', scaling_factors, warmth_entry, precision=highest_accuracy)
    means_v = along_latitude_flow / jnp.maximum(watered_total, 1.0)
    averages_heat = along_latitude_warmth / jnp.maximum(watered_total, 1.0)
    bar_v = lax.optimization_barrier(jnp.mean(means_v, axis=0))
    bar_t = lax.optimization_barrier(jnp.mean(averages_heat, axis=0))
    mean_velocity = lax.optimization_barrier(jnp.mean(meridional_speed_layer, axis=0))
    average_warmth = lax.optimization_barrier(jnp.mean(warmth_entry, axis=0))
    bar_v_cells = jnp.einsum('bji,bj->ji', one_hot, bar_v, precision=highest_accuracy)
    averaged_heat_grid = jnp.einsum('bji,bj->ji', one_hot, bar_t, precision=highest_accuracy)
    means_v_cells = jnp.einsum('bji,tbj->tji', one_hot, means_v, precision=highest_accuracy)
    averages_heat_grid = jnp.einsum('bji,tbj->tji', one_hot, averages_heat, precision=highest_accuracy)
    velocity_star = mean_velocity - bar_v_cells
    temp_star = average_warmth - averaged_heat_grid
    velocity_eddy = meridional_speed_layer - mean_velocity - (means_v_cells - bar_v_cells)
    warmth_fluctuation = warmth_entry - average_warmth - (averages_heat_grid - averaged_heat_grid)
    scaling = 1.0 / math.sqrt(LONGITUDE_SLOTS)
    mean_flow = scaling * watered_total * bar_v * bar_t
    steady_share = scaling * jnp.einsum('bji,ji->bj', scaling_factors, velocity_star * temp_star, precision=highest_accuracy)
    zonal_swing = scaling * watered_total * lax.optimization_barrier(jnp.mean((means_v - bar_v) * (averages_heat - bar_t), axis=0))
    transient = scaling * jnp.einsum('bji,ji->bj', scaling_factors, lax.optimization_barrier(jnp.mean(velocity_eddy * warmth_fluctuation, axis=0)), precision=highest_accuracy)
    return (wet_cells * temp_star, jnp.stack([mean_flow, steady_share, zonal_swing, transient]))

def reference(poleward_flow, potential_warmth, water_profile_flag, floor_count, catchment_label_for_site):
    bottom_layer_limit = (water_profile_flag * floor_count).astype(jnp.float32)

    def per_level(layer_position):
        meridional_speed_layer = lax.dynamic_index_in_dim(poleward_flow, layer_position, 1, keepdims=False)
        thermal_layer_slice = lax.dynamic_index_in_dim(potential_warmth, layer_position, 1, keepdims=False)
        return layer_summands(layer_position, meridional_speed_layer, thermal_layer_slice, bottom_layer_limit, catchment_label_for_site)
    eddy_temp, stacked = lax.map(per_level, jnp.arange(LAYERS, dtype=jnp.int32))
    return (eddy_temp, jnp.transpose(stacked, (1, 2, 0, 3)))
```

```python
import functools
import math

import jax
import jax.numpy as jnp
from jax import lax
from jax.experimental import pallas as pl
from jax.experimental.pallas import tpu as pltpu
from jax.sharding import PartitionSpec as P

BASINS = 10
SUB = 8
LANES = 128


def cover(total, unit):
    return -(-total // unit)


def iota(axis):
    return lax.broadcasted_iota(jnp.int32, (SUB, LANES), axis)


def pick_lanes(tiles, start, width):
    first, shift = divmod(start, LANES)
    if shift == 0:
        return tiles[first]
    left = pltpu.roll(tiles[first], LANES - shift, 1)
    if shift + width <= LANES:
        return left
    right = pltpu.roll(tiles[first + 1], LANES - shift, 1)
    return jnp.where(lax.broadcasted_iota(jnp.int32, left.shape, 1) < LANES - shift, left, right)


def place_lanes(blocks, width, count):
    tiles = [None] * count
    lane = lax.broadcasted_iota(jnp.int32, blocks[0].shape, 1)
    for k, block in enumerate(blocks):
        first, shift = divmod(k * width, LANES)
        moved = block if shift == 0 else pltpu.roll(block, shift, 1)
        if tiles[first] is None:
            tiles[first] = moved
        else:
            tiles[first] = jnp.where(lane < shift, tiles[first], moved)
        if shift + width > LANES:
            tiles[first + 1] = moved
    return tiles


def sums_kernel(
    dims, flow, warmth, flag, floor, basin, halo, out, mean_warmth, limit,
    flow_buf, warmth_buf, depth_buf, flow_sem, warmth_sem,
):
    snapshots, levels, rows, blocks, tiles, dests, per_dest = dims
    width = BASINS * SUB
    quantities = 2 * snapshots + 4
    own_rows = tiles * quantities

    def flow_copy(n):
        at = pl.ds(pl.multiple_of(n * SUB, SUB), SUB)
        return pltpu.make_async_copy(flow.at[:, :, at, :], flow_buf.at[:, :, at, :], flow_sem.at[n])

    def warmth_copy(n):
        at = pl.ds(pl.multiple_of(n * SUB, SUB), SUB)
        return pltpu.make_async_copy(
            warmth.at[:, :, at, :], warmth_buf.at[:, :, at, :], warmth_sem.at[n]
        )

    for n in range(blocks):
        warmth_copy(n).start()
        flow_copy(n).start()
    for t in range(snapshots):
        for k in range(levels):
            n = t * levels + k
            warmth_buf[t, k, rows : rows + 1, :] = halo[n : n + 1, :]
    depth_buf[0:rows, :] = (flag[...] * floor[...]).astype(jnp.float32)
    depth_buf[rows : rows + 1, :] = halo[snapshots * levels : snapshots * levels + 1, :]
    warmth_copy(0).wait()

    sub, lane = iota(0), iota(1)
    diagonal = lane % SUB

    def one_block(n, last):
        at = pl.multiple_of(n * SUB, SUB)
        if not last:
            warmth_copy(n + 1).wait()
        flow_copy(n).wait()
        shallow = jnp.minimum(depth_buf[pl.ds(at, SUB), :], depth_buf[pl.ds(at + 1, SUB), :])
        limit[pl.ds(at, SUB), :] = shallow
        label = basin[pl.ds(at, SUB), :]
        placed = []
        for k in range(levels):
            v = [flow_buf[t, k, pl.ds(at, SUB), :] for t in range(snapshots)]
            w = [
                0.5 * (warmth_buf[t, k, pl.ds(at, SUB), :] + warmth_buf[t, k, pl.ds(at + 1, SUB), :])
                for t in range(snapshots)
            ]
            mv = sum(v[1:], v[0]) * (1.0 / snapshots)
            mw = sum(w[1:], w[0]) * (1.0 / snapshots)
            cross = sum((a - mv) * (b - mw) for a, b in zip(v, w)) * (1.0 / snapshots)
            mean_warmth[k, pl.ds(at, SUB), :] = mw
            data = jnp.concatenate(v + w + [mv * mw, cross, mw, jnp.ones_like(mw)], axis=0)
            masked = jnp.where(shallow > float(k), label, -1)
            hot = jnp.concatenate(
                [jnp.where(masked == b, 1.0, 0.0) for b in range(BASINS)], axis=0
            ).astype(jnp.bfloat16)
            total = None
            rest = data
            for piece in range(3):
                part = rest.astype(jnp.bfloat16)
                if piece < 2:
                    rest = rest - part.astype(jnp.float32)
                dot = lax.dot_general(
                    part, hot, (((1,), (1,)), ((), ())), preferred_element_type=jnp.float32
                )
                total = dot if total is None else total + dot
            total = jnp.concatenate(
                [total, jnp.zeros((total.shape[0], LANES - width), jnp.float32)], axis=1
            )
            groups = []
            for g in range(quantities // SUB):
                acc = None
                for s in range(SUB):
                    q = g * SUB + s
                    row = jnp.take_along_axis(
                        total[q * SUB : (q + 1) * SUB], diagonal, axis=0, mode="promise_in_bounds"
                    )
                    acc = row if acc is None else jnp.where(sub == s, row, acc)
                groups.append(acc)
            placed.append(jnp.concatenate(groups, axis=0))
        done = place_lanes(placed, width, tiles)
        dest, inner = (n // per_dest, n % per_dest) if per_dest > 1 else (n, 0)
        for c in range(tiles):
            base = inner * own_rows + c * quantities
            out[dest, pl.ds(pl.multiple_of(base, SUB), quantities), :] = done[c]
            for q in range(2):
                row = per_dest * own_rows + (c * 2 + q) * blocks + n
                out[0, pl.ds(row, 1), :] = done[c][quantities - 2 + q : quantities - 1 + q]

    def body(n, carry):
        one_block(n, False)
        return carry

    lax.fori_loop(0, blocks - 1, body, 0)
    one_block(blocks - 1, True)
    for d in range(1, dests):
        out[d, per_dest * own_rows :, :] = out[0, per_dest * own_rows :, :]


def finish_kernel(dims, scaling, got, mean_warmth, limit, basin, eddy, transport):
    snapshots, levels, rows, blocks, tiles, dests, per_dest = dims
    width = BASINS * SUB
    quantities = 2 * snapshots + 4
    own_rows = tiles * quantities
    sub, lane = iota(0), iota(1)
    mine = got[0]
    for d in range(1, got.shape[0]):
        mine = mine + got[d]
    shared = mine[per_dest * own_rows :]
    bar = []
    for c in range(tiles):
        at = c * 2 * blocks
        bar.append(shared[at : at + blocks] / jnp.maximum(shared[at + blocks : at + 2 * blocks], 1.0))
    for k in range(levels):
        level = pick_lanes(bar, k * width, width)
        for n in range(blocks):
            where = basin[n * SUB : (n + 1) * SUB, :] * SUB + sub
            row = jnp.broadcast_to(level[n : n + 1], (SUB, LANES))
            cell = jnp.take_along_axis(row, where, axis=1, mode="promise_in_bounds")
            deep = limit[n * SUB : (n + 1) * SUB, :] > float(k)
            star = mean_warmth[k, n * SUB : (n + 1) * SUB, :] - cell
            eddy[k, n * SUB : (n + 1) * SUB, :] = jnp.where(deep, star, 0.0)
    spread = jnp.minimum(lane, BASINS - 1) * SUB + sub
    for i in range(per_dest):
        terms = []
        for c in range(tiles):
            own = mine[i * own_rows + c * quantities : i * own_rows + (c + 1) * quantities]
            count = own[quantities - 1 : quantities]
            floor = jnp.maximum(count, 1.0)
            v = own[:snapshots] / floor
            w = own[snapshots : 2 * snapshots] / floor
            bar_v = jnp.sum(v, axis=0, keepdims=True) * (1.0 / snapshots)
            bar_w = jnp.sum(w, axis=0, keepdims=True) * (1.0 / snapshots)
            swing = jnp.sum((v - bar_v) * (w - bar_w), axis=0, keepdims=True) * (1.0 / snapshots)
            mean_part = count * bar_v * bar_w
            swing = count * swing
            product = own[2 * snapshots : 2 * snapshots + 1]
            cross = own[2 * snapshots + 1 : 2 * snapshots + 2]
            four = [mean_part, product - mean_part, swing, cross - swing]
            terms.append(scaling * jnp.concatenate(four + four, axis=0))
        for k in range(levels):
            level = pick_lanes(terms, k * width, width)
            for term in range(4):
                row = jnp.broadcast_to(level[term : term + 1], (SUB, LANES))
                cell = jnp.take_along_axis(row, spread, axis=1, mode="promise_in_bounds")
                transport[term, k, i * SUB : (i + 1) * SUB, :] = cell[:, :BASINS]


def shards(flow, warmth, flag, floor, basin):
    snapshots, levels, rows, cols = flow.shape
    lon, lat = lax.axis_size("lon"), lax.axis_size("lat")
    scaling = 1.0 / math.sqrt(cols * lon)
    share = rows // lon
    blocks = rows // SUB
    per_dest = max(1, share // SUB)
    dests = blocks // per_dest
    width = BASINS * SUB
    tiles = cover(levels * width, LANES)
    quantities = 2 * snapshots + 4
    dims = (snapshots, levels, rows, blocks, tiles, dests, per_dest)
    chunk = per_dest * tiles * quantities + tiles * 2 * blocks

    edge = jnp.concatenate(
        [
            warmth[:, :, 0, :].reshape(snapshots * levels, cols),
            (flag[:1] * floor[:1]).astype(jnp.float32),
        ],
        axis=0,
    )
    halo = lax.ppermute(edge, "lat", [(i, i - 1) for i in range(1, lat)])

    vmem = pl.BlockSpec(memory_space=pltpu.VMEM)
    hbm = pl.BlockSpec(memory_space=pl.ANY)
    sent, mean_warmth, limit = pl.pallas_call(
        functools.partial(sums_kernel, dims),
        out_shape=(
            jax.ShapeDtypeStruct((dests, chunk, LANES), jnp.float32),
            jax.ShapeDtypeStruct((levels, rows, cols), jnp.float32),
            jax.ShapeDtypeStruct((rows, cols), jnp.float32),
        ),
        in_specs=[hbm, hbm, vmem, vmem, vmem, vmem],
        out_specs=(vmem, vmem, vmem),
        scratch_shapes=[
            pltpu.VMEM((snapshots, levels, rows, cols), jnp.float32),
            pltpu.VMEM((snapshots, levels, rows + SUB, cols), jnp.float32),
            pltpu.VMEM((rows + SUB, cols), jnp.float32),
            pltpu.SemaphoreType.DMA((blocks,)),
            pltpu.SemaphoreType.DMA((blocks,)),
        ],
        name="basin_sums",
    )(flow, warmth, flag, floor, basin, halo)

    if dests != lon:
        sent = jnp.repeat(sent, lon // dests, axis=0, total_repeat_length=lon)
    got = lax.all_to_all(sent, "lon", 0, 0)

    eddy, transport = pl.pallas_call(
        functools.partial(finish_kernel, dims, scaling),
        out_shape=(
            jax.ShapeDtypeStruct((levels, rows, cols), jnp.float32),
            jax.ShapeDtypeStruct((4, levels, per_dest * SUB, BASINS), jnp.float32),
        ),
        in_specs=[vmem, vmem, vmem, vmem],
        out_specs=(vmem, vmem),
        name="finish",
    )(got, mean_warmth, limit, basin)
    if dests != lon:
        first = lax.axis_index("lon") * share % SUB
        transport = lax.dynamic_slice_in_dim(transport, first, share, 2)
    return eddy, jnp.transpose(transport, (0, 3, 1, 2))


def solution(mesh):
    return jax.shard_map(
        shards,
        mesh=mesh,
        in_specs=(
            P(None, None, "lat", "lon"),
            P(None, None, "lat", "lon"),
            P("lat", "lon"),
            P("lat", "lon"),
            P("lat", "lon"),
        ),
        out_specs=(P(None, "lat", "lon"), P(None, None, None, ("lat", "lon"))),
        check_vma=False,
    )
```

```python
import functools
import math

import jax
import jax.numpy as jnp
from jax import lax
from jax.experimental import pallas as pl
from jax.experimental.pallas import tpu as pltpu
from jax.sharding import PartitionSpec as P

BASINS = 10
SUB = 8
LANES = 128
GRANT = 16 * 1024 * 1024


def cover(total, unit):
    return -(-total // unit)


def iota(axis):
    return lax.broadcasted_iota(jnp.int32, (SUB, LANES), axis)


def pick_lanes(tiles, start, width):
    first, shift = divmod(start, LANES)
    if shift == 0:
        return tiles[first]
    left = pltpu.roll(tiles[first], LANES - shift, 1)
    if shift + width <= LANES:
        return left
    right = pltpu.roll(tiles[first + 1], LANES - shift, 1)
    return jnp.where(lax.broadcasted_iota(jnp.int32, left.shape, 1) < LANES - shift, left, right)


def place_lanes(blocks, width, count):
    tiles = [None] * count
    lane = lax.broadcasted_iota(jnp.int32, blocks[0].shape, 1)
    for k, block in enumerate(blocks):
        first, shift = divmod(k * width, LANES)
        moved = block if shift == 0 else pltpu.roll(block, shift, 1)
        if tiles[first] is None:
            tiles[first] = moved
        else:
            tiles[first] = jnp.where(lane < shift, tiles[first], moved)
        if shift + width > LANES:
            tiles[first + 1] = moved
    return tiles


def edge_kernel(dims, warmth, flag, floor, edge, rows_buf, flag_buf, floor_buf, sem):
    snapshots, levels = dims[:2]
    first = slice(0, SUB)
    copies = [
        pltpu.make_async_copy(flag.at[first, :], flag_buf, sem.at[snapshots]),
        pltpu.make_async_copy(floor.at[first, :], floor_buf, sem.at[snapshots + 1]),
    ] + [
        pltpu.make_async_copy(warmth.at[t, :, first, :], rows_buf.at[t], sem.at[t])
        for t in range(snapshots)
    ]
    for copy in copies:
        copy.start()
    for copy in copies:
        copy.wait()
    depth = (flag_buf[0:1, :] * floor_buf[0:1, :]).astype(jnp.float32)
    edge[snapshots * levels : snapshots * levels + 1, :] = depth
    for t in range(snapshots):
        for k in range(levels):
            edge[t * levels + k : t * levels + k + 1, :] = rows_buf[t, k, 0:1, :]


def block_sums(dims, n, get_v, get_w, shallow, label, put_own, put_shared, put_mean):
    snapshots, levels, rows, blocks, tiles, dests, per_dest = dims
    width = BASINS * SUB
    quantities = 2 * snapshots + 4
    own_rows = tiles * quantities
    sub, lane = iota(0), iota(1)
    diagonal = lane % SUB
    placed = []
    for k in range(levels):
        v = [get_v(t, k) for t in range(snapshots)]
        w = [get_w(t, k) for t in range(snapshots)]
        mv = sum(v[1:], v[0]) * (1.0 / snapshots)
        mw = sum(w[1:], w[0]) * (1.0 / snapshots)
        cross = sum((a - mv) * (b - mw) for a, b in zip(v, w)) * (1.0 / snapshots)
        put_mean(k, mw)
        data = jnp.concatenate(v + w + [mv * mw, cross, mw, jnp.ones_like(mw)], axis=0)
        masked = jnp.where(shallow > float(k), label, -1)
        hot = jnp.concatenate(
            [jnp.where(masked == b, 1.0, 0.0) for b in range(BASINS)], axis=0
        ).astype(jnp.bfloat16)
        total = None
        rest = data
        for piece in range(3):
            part = rest.astype(jnp.bfloat16)
            if piece < 2:
                rest = rest - part.astype(jnp.float32)
            dot = lax.dot_general(
                part, hot, (((1,), (1,)), ((), ())), preferred_element_type=jnp.float32
            )
            total = dot if total is None else total + dot
        total = jnp.concatenate(
            [total, jnp.zeros((total.shape[0], LANES - width), jnp.float32)], axis=1
        )
        groups = []
        for g in range(quantities // SUB):
            acc = None
            for s in range(SUB):
                q = g * SUB + s
                row = jnp.take_along_axis(
                    total[q * SUB : (q + 1) * SUB], diagonal, axis=0, mode="promise_in_bounds"
                )
                acc = row if acc is None else jnp.where(sub == s, row, acc)
            groups.append(acc)
        placed.append(jnp.concatenate(groups, axis=0))
    done = place_lanes(placed, width, tiles)
    for c in range(tiles):
        put_own(c, done[c])
        for q in range(2):
            put_shared(c * 2 + q, done[c][quantities - 2 + q : quantities - 1 + q])


def writers(dims, n, keep, give):
    snapshots, levels, rows, blocks, tiles, dests, per_dest = dims
    quantities = 2 * snapshots + 4
    own_rows = tiles * quantities
    dest, inner = (n // per_dest, n % per_dest) if per_dest > 1 else (n, 0)
    halves = (keep,) if give is None else (keep, give)
    half = dest if give is None else dest // 2
    shared_at = keep.shape[0] - 2 * tiles * blocks

    def put_own(c, value):
        base = (half * per_dest + inner) * own_rows + c * quantities
        if not isinstance(base, int):
            base = pl.multiple_of(base, SUB)
        at = pl.ds(base, quantities)
        if give is None:
            keep[at, :] = value
            return
        mine = lax.axis_index("lon") % 2 == dest % 2

        @pl.when(mine)
        def _():
            keep[at, :] = value

        @pl.when(jnp.logical_not(mine))
        def _():
            give[at, :] = value

    def put_shared(place, value):
        for ref in halves:
            ref[pl.ds(shared_at + place * blocks + n, 1), :] = value

    return put_own, put_shared


def inner_kernel(dims, pairs, flow, warmth, flag, floor, basin, *outs):
    rows, blocks = dims[2:4]
    keep, give = outs[:2] if pairs else (outs[0], None)
    mean_warmth, limit, depth_buf = outs[-3:]
    depth_buf[...] = (flag[...] * floor[...]).astype(jnp.float32)

    def body(n, carry):
        at = pl.multiple_of(n * SUB, SUB)
        here, north = pl.ds(at, SUB), pl.ds(at + 1, SUB)
        shallow = jnp.minimum(depth_buf[here, :], depth_buf[north, :])
        limit[here, :] = shallow

        def put_mean(k, value):
            mean_warmth[k, here, :] = value

        def get_v(t, k):
            return flow[t, k, here, :]

        def get_w(t, k):
            return 0.5 * (warmth[t, k, here, :] + warmth[t, k, north, :])

        put_own, put_shared = writers(dims, n, keep, give)
        block_sums(
            dims, n, get_v, get_w, shallow, basin[here, :], put_own, put_shared, put_mean
        )
        return carry

    lax.fori_loop(0, blocks - 1, body, 0)


def last_kernel(dims, pairs, halo, flow, warmth, flag, floor, basin, *refs):
    snapshots, levels, rows, blocks = dims[:4]
    outs = refs[len(refs) // 2 :]
    keep, give = outs[:2] if pairs else (outs[0], None)
    mean_warmth, limit = outs[-2:]
    here = slice(rows - SUB, rows)
    below = lax.broadcasted_iota(jnp.int32, (SUB, LANES), 0) < SUB - 1

    def north(block, edge_row):
        return jnp.where(below, pltpu.roll(block, SUB - 1, 0), edge_row)

    depth = (flag[here, :] * floor[here, :]).astype(jnp.float32)
    edge_at = snapshots * levels
    shallow = jnp.minimum(depth, north(depth, halo[edge_at : edge_at + 1, :]))
    limit[here, :] = shallow

    def put_mean(k, value):
        mean_warmth[k, here, :] = value

    def get_v(t, k):
        return flow[t, k, here, :]

    def get_w(t, k):
        block = warmth[t, k, here, :]
        n = t * levels + k
        return 0.5 * (block + north(block, halo[n : n + 1, :]))

    put_own, put_shared = writers(dims, blocks - 1, keep, give)
    block_sums(
        dims, blocks - 1, get_v, get_w, shallow, basin[here, :], put_own, put_shared, put_mean
    )


def pair_kernel(dims, keep, came, *outs):
    tiles, per_dest = dims[4], dims[6]
    own_rows = per_dest * tiles * (2 * dims[0] + 4)
    chips = len(outs)
    shared = chips * own_rows
    chip = lax.axis_index("lon") // 2
    for offset, out in enumerate(outs):
        at = pl.multiple_of((chip ^ offset) * own_rows, SUB)
        out[0:own_rows, :] = keep[pl.ds(at, own_rows), :] + came[pl.ds(at, own_rows), :]
        out[own_rows:, :] = keep[shared:, :] + came[shared:, :]


def finish_kernel(dims, scaling, *refs):
    mean_warmth, limit, basin, eddy, transport = refs[-5:]
    snapshots, levels, rows, blocks, tiles, dests, per_dest = dims
    width = BASINS * SUB
    quantities = 2 * snapshots + 4
    own_rows = tiles * quantities
    sub, lane = iota(0), iota(1)
    got = refs[:-5]
    if len(got) == 1:
        got = [got[0].at[d] for d in range(got[0].shape[0])]
    mine = got[0][...]
    for part in got[1:]:
        mine = mine + part[...]
    shared = mine[per_dest * own_rows :]
    bar = []
    for c in range(tiles):
        at = c * 2 * blocks
        bar.append(shared[at : at + blocks] / jnp.maximum(shared[at + blocks : at + 2 * blocks], 1.0))
    for k in range(levels):
        level = pick_lanes(bar, k * width, width)
        for n in range(blocks):
            where = basin[n * SUB : (n + 1) * SUB, :] * SUB + sub
            row = jnp.broadcast_to(level[n : n + 1], (SUB, LANES))
            cell = jnp.take_along_axis(row, where, axis=1, mode="promise_in_bounds")
            deep = limit[n * SUB : (n + 1) * SUB, :] > float(k)
            star = mean_warmth[k, n * SUB : (n + 1) * SUB, :] - cell
            eddy[k, n * SUB : (n + 1) * SUB, :] = jnp.where(deep, star, 0.0)
    spread = jnp.minimum(lane, BASINS - 1) * SUB + sub
    for i in range(per_dest):
        terms = []
        for c in range(tiles):
            own = mine[i * own_rows + c * quantities : i * own_rows + (c + 1) * quantities]
            count = own[quantities - 1 : quantities]
            floor = jnp.maximum(count, 1.0)
            v = own[:snapshots] / floor
            w = own[snapshots : 2 * snapshots] / floor
            bar_v = jnp.sum(v, axis=0, keepdims=True) * (1.0 / snapshots)
            bar_w = jnp.sum(w, axis=0, keepdims=True) * (1.0 / snapshots)
            swing = jnp.sum((v - bar_v) * (w - bar_w), axis=0, keepdims=True) * (1.0 / snapshots)
            mean_part = count * bar_v * bar_w
            swing = count * swing
            product = own[2 * snapshots : 2 * snapshots + 1]
            cross = own[2 * snapshots + 1 : 2 * snapshots + 2]
            four = [mean_part, product - mean_part, swing, cross - swing]
            terms.append(scaling * jnp.concatenate(four + four, axis=0))
        for k in range(levels):
            level = pick_lanes(terms, k * width, width)
            for term in range(4):
                row = jnp.broadcast_to(level[term : term + 1], (SUB, LANES))
                cell = jnp.take_along_axis(row, spread, axis=1, mode="promise_in_bounds")
                transport[term, k, i * SUB : (i + 1) * SUB, :] = cell[:, :BASINS]


def shards(flow, warmth, flag, floor, basin):
    snapshots, levels, rows, cols = flow.shape
    lon, lat = lax.axis_size("lon"), lax.axis_size("lat")
    scaling = 1.0 / math.sqrt(cols * lon)
    share = rows // lon
    blocks = rows // SUB
    per_dest = max(1, share // SUB)
    dests = blocks // per_dest
    width = BASINS * SUB
    tiles = cover(levels * width, LANES)
    quantities = 2 * snapshots + 4
    dims = (snapshots, levels, rows, blocks, tiles, dests, per_dest)
    own_rows, shared_rows = per_dest * tiles * quantities, tiles * 2 * blocks
    pairs = dests == lon and lon in (2, 4, 8)

    vmem = pl.BlockSpec(memory_space=pltpu.VMEM)
    hbm = pl.BlockSpec(memory_space=pl.ANY)
    params = pltpu.CompilerParams(vmem_limit_bytes=GRANT)

    def near(x):
        return pltpu.with_memory_space_constraint(x, pltpu.VMEM)

    def far(x):
        return pltpu.with_memory_space_constraint(x, pltpu.HBM)

    edge = pl.pallas_call(
        functools.partial(edge_kernel, dims),
        out_shape=pltpu.VMEM((snapshots * levels + 1, cols), jnp.float32),
        in_specs=[hbm] * 3,
        out_specs=vmem,
        scratch_shapes=[
            pltpu.VMEM((snapshots, levels, SUB, cols), jnp.float32),
            pltpu.VMEM((SUB, cols), jnp.int32),
            pltpu.VMEM((SUB, cols), jnp.int32),
            pltpu.SemaphoreType.DMA((snapshots + 2,)),
        ],
        compiler_params=params,
        cost_estimate=pl.CostEstimate(flops=10000000000, bytes_accessed=8 << 20, transcendentals=0),
        name="edge",
    )(far(warmth), far(flag), far(floor))
    halo = lax.ppermute(edge, "lat", [(i, i - 1) for i in range(1, lat)])

    flow, warmth, flag, floor, basin = (near(x) for x in (flow, warmth, flag, floor, basin))
    half = pltpu.VMEM((dests // 2 * own_rows + shared_rows, LANES), jnp.float32)
    full = pltpu.VMEM((dests * own_rows + shared_rows, LANES), jnp.float32)
    results = ((half, half) if pairs else (full,)) + (
        pltpu.VMEM((levels, rows, cols), jnp.float32),
        pltpu.VMEM((rows, cols), jnp.float32),
    )
    sums = pl.pallas_call(
        functools.partial(inner_kernel, dims, pairs),
        out_shape=results,
        in_specs=[vmem] * 5,
        out_specs=(vmem,) * len(results),
        scratch_shapes=[pltpu.VMEM((rows, cols), jnp.float32)],
        compiler_params=params,
        name="inner_rows",
    )(flow, warmth, flag, floor, basin)
    sums = pl.pallas_call(
        functools.partial(last_kernel, dims, pairs),
        out_shape=results,
        in_specs=[vmem] * (6 + len(results)),
        out_specs=(vmem,) * len(results),
        input_output_aliases={6 + i: i for i in range(len(results))},
        compiler_params=params,
        name="last_rows",
    )(halo, flow, warmth, flag, floor, basin, *sums)
    mean_warmth, limit = sums[-2:]

    if pairs:
        keep, give = sums[:2]
        came = lax.ppermute(give, "lon", [(i, i ^ 1) for i in range(lon)])
        message = pltpu.VMEM((own_rows + shared_rows, LANES), jnp.float32)
        chips = lon // 2
        messages = pl.pallas_call(
            functools.partial(pair_kernel, dims),
            out_shape=(message,) * chips,
            in_specs=[vmem, vmem],
            out_specs=(vmem,) * chips,
            compiler_params=params,
            name="pair_sums",
        )(keep, came)
        got = messages[:1] + tuple(
            lax.ppermute(messages[m], "lon", [(i, i ^ (2 * m)) for i in range(lon)])
            for m in range(1, chips)
        )
    else:
        own, shared = sums[0][: dests * own_rows], sums[0][dests * own_rows :]
        sent = jnp.concatenate(
            [own.reshape(dests, own_rows, LANES), jnp.broadcast_to(shared, (dests, shared_rows, LANES))],
            axis=1,
        )
        if dests != lon:
            sent = jnp.repeat(sent, lon // dests, axis=0, total_repeat_length=lon)
        got = (lax.all_to_all(sent, "lon", 0, 0),)

    eddy, transport = pl.pallas_call(
        functools.partial(finish_kernel, dims, scaling),
        out_shape=(
            jax.ShapeDtypeStruct((levels, rows, cols), jnp.float32),
            jax.ShapeDtypeStruct((4, levels, per_dest * SUB, BASINS), jnp.float32),
        ),
        in_specs=[vmem] * (len(got) + 3),
        out_specs=(vmem, vmem),
        compiler_params=params,
        name="finish",
    )(*got, mean_warmth, limit, basin)
    if dests != lon:
        first = lax.axis_index("lon") * share % SUB
        transport = lax.dynamic_slice_in_dim(transport, first, share, 2)
    return eddy, jnp.transpose(transport, (0, 3, 1, 2))


def solution(mesh):
    return jax.shard_map(
        shards,
        mesh=mesh,
        in_specs=(
            P(None, None, "lat", "lon"),
            P(None, None, "lat", "lon"),
            P("lat", "lon"),
            P("lat", "lon"),
            P("lat", "lon"),
        ),
        out_specs=(P(None, "lat", "lon"), P(None, None, None, ("lat", "lon"))),
        check_vma=False,
    )
```

```python
import functools
import math

import jax
import jax.numpy as jnp
from jax import lax
from jax.experimental import pallas as pl
from jax.experimental.pallas import tpu as pltpu
from jax.sharding import PartitionSpec as P

BASINS = 10
SUB = 8
LANES = 128
GRANT = 16 * 1024 * 1024


def cover(total, unit):
    return -(-total // unit)


def iota(axis):
    return lax.broadcasted_iota(jnp.int32, (SUB, LANES), axis)


def pick_lanes(tiles, start, width):
    first, shift = divmod(start, LANES)
    if shift == 0:
        return tiles[first]
    left = pltpu.roll(tiles[first], LANES - shift, 1)
    if shift + width <= LANES:
        return left
    right = pltpu.roll(tiles[first + 1], LANES - shift, 1)
    return jnp.where(lax.broadcasted_iota(jnp.int32, left.shape, 1) < LANES - shift, left, right)


def edge_kernel(dims, warmth, flag, floor, edge, rows_buf, flag_buf, floor_buf, sem):
    snapshots, levels = dims[:2]
    first = slice(0, SUB)
    copies = [
        pltpu.make_async_copy(flag.at[first, :], flag_buf, sem.at[snapshots]),
        pltpu.make_async_copy(floor.at[first, :], floor_buf, sem.at[snapshots + 1]),
    ] + [
        pltpu.make_async_copy(warmth.at[t, :, first, :], rows_buf.at[t], sem.at[t])
        for t in range(snapshots)
    ]
    for copy in copies:
        copy.start()
    for copy in copies:
        copy.wait()
    depth = (flag_buf[0:1, :] * floor_buf[0:1, :]).astype(jnp.float32)
    edge[snapshots * levels : snapshots * levels + 1, :] = depth
    for t in range(snapshots):
        for k in range(levels):
            edge[t * levels + k : t * levels + k + 1, :] = rows_buf[t, k, 0:1, :]


def block_sums(dims, n, get_v, get_w, shallow, label, put_own, put_shared, put_mean):
    snapshots, levels, rows, blocks, tiles, dests, per_dest = dims
    width = BASINS * SUB
    quantities = 2 * snapshots + 4
    own_rows = tiles * quantities
    sub, lane = iota(0), iota(1)
    diagonal = lane % SUB

    def level_data(k):
        v = [get_v(t, k) for t in range(snapshots)]
        w = [get_w(t, k) for t in range(snapshots)]
        mv = sum(v[1:], v[0]) * (1.0 / snapshots)
        mw = sum(w[1:], w[0]) * (1.0 / snapshots)
        cross = sum((a - mv) * (b - mw) for a, b in zip(v, w)) * (1.0 / snapshots)
        put_mean(k, mw)
        return jnp.concatenate(v + w + [mv * mw, cross, mw, jnp.ones_like(mw)], axis=0)

    def level_hot(k):
        masked = jnp.where(shallow > float(k), label, -1)
        return [jnp.where(masked == b, 1.0, 0.0) for b in range(BASINS)]

    done = [None] * tiles
    nothing = jnp.zeros((SUB, LANES), jnp.float32)
    for first in range(0, levels, 2):
        pair = range(first, min(first + 2, levels))
        tile, shift = divmod(first * width, LANES)
        data = jnp.concatenate([level_data(k) for k in pair], axis=1)
        pad = [nothing] * (shift // SUB)
        columns = []
        for k in pair:
            column = list(pad)
            for other in pair:
                column += level_hot(k) if other == k else [nothing] * BASINS
            columns.append(jnp.concatenate(column, axis=0))
        hot = jnp.concatenate(columns, axis=1).astype(jnp.bfloat16)
        height = quantities * SUB
        parts = []
        for at in range(0, height, 64):
            rest = data[at : at + 64]
            for piece in range(3):
                parts.append(rest.astype(jnp.bfloat16))
                if piece < 2:
                    rest = rest - parts[-1].astype(jnp.float32)
        dots = lax.dot_general(
            jnp.concatenate(parts, axis=0),
            hot,
            (((1,), (1,)), ((), ())),
            preferred_element_type=jnp.float32,
        )
        sums = []
        for at in range(0, height, 64):
            x = [dots[3 * at + p * 64 : 3 * at + (p + 1) * 64] for p in range(3)]
            sums.append(x[0] + x[1] + x[2])
        total = jnp.concatenate(sums, axis=0)
        spare = -total.shape[1] % LANES
        if spare:
            total = jnp.concatenate(
                [total, jnp.zeros((total.shape[0], spare), jnp.float32)], axis=1
            )
        for c in range(total.shape[1] // LANES):
            groups = []
            for g in range(quantities // SUB):
                acc = None
                for s in range(SUB):
                    q = g * SUB + s
                    row = jnp.take_along_axis(
                        total[q * SUB : (q + 1) * SUB, c * LANES : (c + 1) * LANES],
                        diagonal,
                        axis=0,
                        mode="promise_in_bounds",
                    )
                    acc = row if acc is None else jnp.where(sub == s, row, acc)
                if done[tile + c] is not None:
                    acc = jnp.where(lane < shift, done[tile + c][g * SUB : (g + 1) * SUB], acc)
                groups.append(acc)
            done[tile + c] = jnp.concatenate(groups, axis=0)
    for c in range(tiles):
        put_own(c, done[c])
        for q in range(2):
            put_shared(c * 2 + q, done[c][quantities - 2 + q : quantities - 1 + q])


def writers(dims, n, keep, give):
    snapshots, levels, rows, blocks, tiles, dests, per_dest = dims
    quantities = 2 * snapshots + 4
    own_rows = tiles * quantities
    dest, inner = (n // per_dest, n % per_dest) if per_dest > 1 else (n, 0)
    halves = (keep,) if give is None else (keep, give)
    half = dest if give is None else dest // 2
    shared_at = keep.shape[0] - 2 * tiles * blocks

    def put_own(c, value):
        base = (half * per_dest + inner) * own_rows + c * quantities
        if not isinstance(base, int):
            base = pl.multiple_of(base, SUB)
        at = pl.ds(base, quantities)
        if give is None:
            keep[at, :] = value
            return
        mine = lax.axis_index("lon") % 2 == dest % 2

        @pl.when(mine)
        def _():
            keep[at, :] = value

        @pl.when(jnp.logical_not(mine))
        def _():
            give[at, :] = value

    def put_shared(place, value):
        for ref in halves:
            ref[pl.ds(shared_at + place * blocks + n, 1), :] = value

    return put_own, put_shared


def inner_kernel(dims, pairs, flow, warmth, flag, floor, basin, *outs):
    rows, blocks = dims[2:4]
    keep, give = outs[:2] if pairs else (outs[0], None)
    mean_warmth, limit, depth_buf = outs[-3:]
    depth_buf[...] = (flag[...] * floor[...]).astype(jnp.float32)

    def body(n, carry):
        at = pl.multiple_of(n * SUB, SUB)
        here, north = pl.ds(at, SUB), pl.ds(at + 1, SUB)
        shallow = jnp.minimum(depth_buf[here, :], depth_buf[north, :])
        limit[here, :] = shallow

        def put_mean(k, value):
            mean_warmth[k, here, :] = value

        def get_v(t, k):
            return flow[t, k, here, :]

        def get_w(t, k):
            return 0.5 * (warmth[t, k, here, :] + warmth[t, k, north, :])

        put_own, put_shared = writers(dims, n, keep, give)
        block_sums(
            dims, n, get_v, get_w, shallow, basin[here, :], put_own, put_shared, put_mean
        )
        return carry

    lax.fori_loop(0, blocks - 1, body, 0)


def last_kernel(dims, pairs, odd_halo, even_halo, flow, warmth, flag, floor, basin, *refs):
    snapshots, levels, rows, blocks = dims[:4]
    outs = refs[len(refs) // 2 :]
    keep, give = outs[:2] if pairs else (outs[0], None)
    mean_warmth, limit = outs[-2:]
    here = slice(rows - SUB, rows)
    below = lax.broadcasted_iota(jnp.int32, (SUB, LANES), 0) < SUB - 1

    lat = lax.axis_index("lat")
    even = lat % 2 == 0
    inside = jnp.where(lat < lax.axis_size("lat") - 1, 1.0, 0.0)

    def north(block, n):
        row = jnp.where(even, even_halo[n : n + 1, :], odd_halo[n : n + 1, :]) * inside
        return jnp.where(below, pltpu.roll(block, SUB - 1, 0), row)

    depth = (flag[here, :] * floor[here, :]).astype(jnp.float32)
    edge_at = snapshots * levels
    shallow = jnp.minimum(depth, north(depth, edge_at))
    limit[here, :] = shallow

    def put_mean(k, value):
        mean_warmth[k, here, :] = value

    def get_v(t, k):
        return flow[t, k, here, :]

    def get_w(t, k):
        block = warmth[t, k, here, :]
        return 0.5 * (block + north(block, t * levels + k))

    put_own, put_shared = writers(dims, blocks - 1, keep, give)
    block_sums(
        dims, blocks - 1, get_v, get_w, shallow, basin[here, :], put_own, put_shared, put_mean
    )


def pair_kernel(dims, keep, came, *outs):
    tiles, per_dest = dims[4], dims[6]
    own_rows = per_dest * tiles * (2 * dims[0] + 4)
    chips = len(outs)
    shared = chips * own_rows
    chip = lax.axis_index("lon") // 2
    for offset, out in enumerate(outs):
        at = pl.multiple_of((chip ^ offset) * own_rows, SUB)
        out[0:own_rows, :] = keep[pl.ds(at, own_rows), :] + came[pl.ds(at, own_rows), :]
        out[own_rows:, :] = keep[shared:, :] + came[shared:, :]


def finish_kernel(dims, scaling, *refs):
    mean_warmth, limit, basin, eddy, transport = refs[-5:]
    snapshots, levels, rows, blocks, tiles, dests, per_dest = dims
    width = BASINS * SUB
    quantities = 2 * snapshots + 4
    own_rows = tiles * quantities
    sub, lane = iota(0), iota(1)
    got = refs[:-5]
    if len(got) == 1:
        got = [got[0].at[d] for d in range(got[0].shape[0])]
    mine = got[0][...]
    for part in got[1:]:
        mine = mine + part[...]
    shared = mine[per_dest * own_rows :]
    bar = []
    for c in range(tiles):
        at = c * 2 * blocks
        bar.append(shared[at : at + blocks] / jnp.maximum(shared[at + blocks : at + 2 * blocks], 1.0))
    for k in range(levels):
        level = pick_lanes(bar, k * width, width)
        for n in range(blocks):
            where = basin[n * SUB : (n + 1) * SUB, :] * SUB + sub
            row = jnp.broadcast_to(level[n : n + 1], (SUB, LANES))
            cell = jnp.take_along_axis(row, where, axis=1, mode="promise_in_bounds")
            deep = limit[n * SUB : (n + 1) * SUB, :] > float(k)
            star = mean_warmth[k, n * SUB : (n + 1) * SUB, :] - cell
            eddy[k, n * SUB : (n + 1) * SUB, :] = jnp.where(deep, star, 0.0)
    spread = jnp.minimum(lane, BASINS - 1) * SUB + sub
    for i in range(per_dest):
        terms = []
        for c in range(tiles):
            own = mine[i * own_rows + c * quantities : i * own_rows + (c + 1) * quantities]
            count = own[quantities - 1 : quantities]
            floor = jnp.maximum(count, 1.0)
            v = own[:snapshots] / floor
            w = own[snapshots : 2 * snapshots] / floor
            bar_v = jnp.sum(v, axis=0, keepdims=True) * (1.0 / snapshots)
            bar_w = jnp.sum(w, axis=0, keepdims=True) * (1.0 / snapshots)
            swing = jnp.sum((v - bar_v) * (w - bar_w), axis=0, keepdims=True) * (1.0 / snapshots)
            mean_part = count * bar_v * bar_w
            swing = count * swing
            product = own[2 * snapshots : 2 * snapshots + 1]
            cross = own[2 * snapshots + 1 : 2 * snapshots + 2]
            four = [mean_part, product - mean_part, swing, cross - swing]
            terms.append(scaling * jnp.concatenate(four + four, axis=0))
        for k in range(levels):
            level = pick_lanes(terms, k * width, width)
            for term in range(4):
                row = jnp.broadcast_to(level[term : term + 1], (SUB, LANES))
                cell = jnp.take_along_axis(row, spread, axis=1, mode="promise_in_bounds")
                transport[term, k, i * SUB : (i + 1) * SUB, :] = cell[:, :BASINS]


def neighbours(lat, lon, first):
    route = []
    for i in range(lat):
        other = i + 1 if (i - first) % 2 == 0 else i - 1
        for j in range(lon):
            if 0 <= other < lat:
                target = other * lon + j
            else:
                target = i * lon + (j ^ 1 if lon % 2 == 0 else j)
            route.append((i * lon + j, target))
    return route


def shards(flow, warmth, flag, floor, basin):
    snapshots, levels, rows, cols = flow.shape
    lon, lat = lax.axis_size("lon"), lax.axis_size("lat")
    scaling = 1.0 / math.sqrt(cols * lon)
    share = rows // lon
    blocks = rows // SUB
    per_dest = max(1, share // SUB)
    dests = blocks // per_dest
    width = BASINS * SUB
    tiles = cover(levels * width, LANES)
    quantities = 2 * snapshots + 4
    dims = (snapshots, levels, rows, blocks, tiles, dests, per_dest)
    own_rows, shared_rows = per_dest * tiles * quantities, tiles * 2 * blocks
    pairs = dests == lon and lon in (2, 4, 8)

    vmem = pl.BlockSpec(memory_space=pltpu.VMEM)
    hbm = pl.BlockSpec(memory_space=pl.ANY)
    params = pltpu.CompilerParams(vmem_limit_bytes=GRANT)

    def near(x):
        return pltpu.with_memory_space_constraint(x, pltpu.VMEM)

    def far(x):
        return pltpu.with_memory_space_constraint(x, pltpu.HBM)

    edge = pl.pallas_call(
        functools.partial(edge_kernel, dims),
        out_shape=pltpu.VMEM((snapshots * levels + 1, cols), jnp.float32),
        in_specs=[hbm] * 3,
        out_specs=vmem,
        scratch_shapes=[
            pltpu.VMEM((snapshots, levels, SUB, cols), jnp.float32),
            pltpu.VMEM((SUB, cols), jnp.int32),
            pltpu.VMEM((SUB, cols), jnp.int32),
            pltpu.SemaphoreType.DMA((snapshots + 2,)),
        ],
        compiler_params=params,
        cost_estimate=pl.CostEstimate(flops=10000000000, bytes_accessed=8 << 20, transcendentals=0),
        name="edge",
    )(far(warmth), far(flag), far(floor))
    halos = tuple(
        lax.ppermute(edge, ("lat", "lon"), neighbours(lat, lon, first)) for first in range(2)
    )

    flow, warmth, flag, floor, basin = (near(x) for x in (flow, warmth, flag, floor, basin))
    half = pltpu.VMEM((dests // 2 * own_rows + shared_rows, LANES), jnp.float32)
    full = pltpu.VMEM((dests * own_rows + shared_rows, LANES), jnp.float32)
    results = ((half, half) if pairs else (full,)) + (
        pltpu.VMEM((levels, rows, cols), jnp.float32),
        pltpu.VMEM((rows, cols), jnp.float32),
    )
    sums = pl.pallas_call(
        functools.partial(inner_kernel, dims, pairs),
        out_shape=results,
        in_specs=[vmem] * 5,
        out_specs=(vmem,) * len(results),
        scratch_shapes=[pltpu.VMEM((rows, cols), jnp.float32)],
        compiler_params=params,
        name="inner_rows",
    )(flow, warmth, flag, floor, basin)
    sums = pl.pallas_call(
        functools.partial(last_kernel, dims, pairs),
        out_shape=results,
        in_specs=[vmem] * (7 + len(results)),
        out_specs=(vmem,) * len(results),
        input_output_aliases={7 + i: i for i in range(len(results))},
        compiler_params=params,
        name="last_rows",
    )(*halos[::-1], flow, warmth, flag, floor, basin, *sums)
    mean_warmth, limit = sums[-2:]

    if pairs:
        keep, give = sums[:2]
        came = lax.ppermute(give, "lon", [(i, i ^ 1) for i in range(lon)])
        message = pltpu.VMEM((own_rows + shared_rows, LANES), jnp.float32)
        chips = lon // 2
        messages = pl.pallas_call(
            functools.partial(pair_kernel, dims),
            out_shape=(message,) * chips,
            in_specs=[vmem, vmem],
            out_specs=(vmem,) * chips,
            compiler_params=params,
            name="pair_sums",
        )(keep, came)
        got = messages[:1] + tuple(
            lax.ppermute(messages[m], "lon", [(i, i ^ (2 * m)) for i in range(lon)])
            for m in reversed(range(1, chips))
        )
    else:
        own, shared = sums[0][: dests * own_rows], sums[0][dests * own_rows :]
        sent = jnp.concatenate(
            [own.reshape(dests, own_rows, LANES), jnp.broadcast_to(shared, (dests, shared_rows, LANES))],
            axis=1,
        )
        if dests != lon:
            sent = jnp.repeat(sent, lon // dests, axis=0, total_repeat_length=lon)
        got = (lax.all_to_all(sent, "lon", 0, 0),)

    eddy, transport = pl.pallas_call(
        functools.partial(finish_kernel, dims, scaling),
        out_shape=(
            jax.ShapeDtypeStruct((levels, rows, cols), jnp.float32),
            jax.ShapeDtypeStruct((4, levels, per_dest * SUB, BASINS), jnp.float32),
        ),
        in_specs=[vmem] * (len(got) + 3),
        out_specs=(vmem, vmem),
        compiler_params=params,
        name="finish",
    )(*got, mean_warmth, limit, basin)
    if dests != lon:
        first = lax.axis_index("lon") * share % SUB
        transport = lax.dynamic_slice_in_dim(transport, first, share, 2)
    return eddy, jnp.transpose(transport, (0, 3, 1, 2))


def solution(mesh):
    return jax.shard_map(
        shards,
        mesh=mesh,
        in_specs=(
            P(None, None, "lat", "lon"),
            P(None, None, "lat", "lon"),
            P("lat", "lon"),
            P("lat", "lon"),
            P("lat", "lon"),
        ),
        out_specs=(P(None, "lat", "lon"), P(None, None, None, ("lat", "lon"))),
        check_vma=False,
    )
```

```python
import functools
import math

import jax
import jax.numpy as jnp
from jax import lax
from jax.experimental import pallas as pl
from jax.experimental.pallas import tpu as pltpu
from jax.sharding import PartitionSpec as P

BASINS = 10
SUB = 8
LANES = 128
GRANT = 16 * 1024 * 1024


def cover(total, unit):
    return -(-total // unit)


def iota(axis):
    return lax.broadcasted_iota(jnp.int32, (SUB, LANES), axis)


def pick_lanes(tiles, start, width):
    first, shift = divmod(start, LANES)
    if shift == 0:
        return tiles[first]
    left = pltpu.roll(tiles[first], LANES - shift, 1)
    if shift + width <= LANES:
        return left
    right = pltpu.roll(tiles[first + 1], LANES - shift, 1)
    return jnp.where(lax.broadcasted_iota(jnp.int32, left.shape, 1) < LANES - shift, left, right)


def edge_kernel(dims, warmth, flag, floor, edge, rows_buf, flag_buf, floor_buf, sem):
    snapshots, levels = dims[:2]
    first = slice(0, SUB)
    copies = [
        pltpu.make_async_copy(flag.at[first, :], flag_buf, sem.at[snapshots]),
        pltpu.make_async_copy(floor.at[first, :], floor_buf, sem.at[snapshots + 1]),
    ] + [
        pltpu.make_async_copy(warmth.at[t, :, first, :], rows_buf.at[t], sem.at[t])
        for t in range(snapshots)
    ]
    for copy in copies:
        copy.start()
    for copy in copies:
        copy.wait()
    depth = (flag_buf[0:1, :] * floor_buf[0:1, :]).astype(jnp.float32)
    edge[snapshots * levels : snapshots * levels + 1, :] = depth
    for t in range(snapshots):
        for k in range(levels):
            edge[t * levels + k : t * levels + k + 1, :] = rows_buf[t, k, 0:1, :]


def block_sums(dims, n, get_v, get_w, shallow, label, put_own, put_shared, put_mean):
    snapshots, levels, rows, blocks, tiles, dests, per_dest = dims
    width = BASINS * SUB
    quantities = 2 * snapshots + 4
    own_rows = tiles * quantities
    sub, lane = iota(0), iota(1)
    diagonal = lane % SUB

    def level_data(k):
        v = [get_v(t, k) for t in range(snapshots)]
        w = [get_w(t, k) for t in range(snapshots)]
        mv = sum(v[1:], v[0]) * (1.0 / snapshots)
        mw = sum(w[1:], w[0]) * (1.0 / snapshots)
        cross = sum((a - mv) * (b - mw) for a, b in zip(v, w)) * (1.0 / snapshots)
        put_mean(k, mw)
        return jnp.concatenate(v + w + [mv * mw, cross, mw, jnp.ones_like(mw)], axis=0)

    def level_hot(k):
        masked = jnp.where(shallow > float(k), label, -1)
        return [jnp.where(masked == b, 1.0, 0.0) for b in range(BASINS)]

    done = [None] * tiles
    nothing = jnp.zeros((SUB, LANES), jnp.float32)
    for first in range(0, levels, 2):
        pair = range(first, min(first + 2, levels))
        tile, shift = divmod(first * width, LANES)
        data = jnp.concatenate([level_data(k) for k in pair], axis=1)
        pad = [nothing] * (shift // SUB)
        columns = []
        for k in pair:
            column = list(pad)
            for other in pair:
                column += level_hot(k) if other == k else [nothing] * BASINS
            columns.append(jnp.concatenate(column, axis=0))
        hot = jnp.concatenate(columns, axis=1).astype(jnp.bfloat16)
        height = quantities * SUB
        exact = 2 * snapshots * SUB
        cuts = [c for c in range(0, exact, 80)] + [exact, height]
        parts, spans = [], []
        for at, end in zip(cuts, cuts[1:]):
            rest = data[at:end]
            count = 2 if at < exact else 3
            for piece in range(count):
                parts.append(rest.astype(jnp.bfloat16))
                if piece < count - 1:
                    rest = rest - parts[-1].astype(jnp.float32)
            spans.append((end - at, count))
        dots = lax.dot_general(
            jnp.concatenate(parts, axis=0),
            hot,
            (((1,), (1,)), ((), ())),
            preferred_element_type=jnp.float32,
        )
        sums, at = [], 0
        for size, count in spans:
            x = dots[at : at + size]
            for piece in range(1, count):
                x = x + dots[at + piece * size : at + (piece + 1) * size]
            sums.append(x)
            at += size * count
        total = jnp.concatenate(sums, axis=0)
        spare = -total.shape[1] % LANES
        if spare:
            total = jnp.concatenate(
                [total, jnp.zeros((total.shape[0], spare), jnp.float32)], axis=1
            )
        for c in range(total.shape[1] // LANES):
            groups = []
            for g in range(quantities // SUB):
                acc = None
                for s in range(SUB):
                    q = g * SUB + s
                    row = jnp.take_along_axis(
                        total[q * SUB : (q + 1) * SUB, c * LANES : (c + 1) * LANES],
                        diagonal,
                        axis=0,
                        mode="promise_in_bounds",
                    )
                    acc = row if acc is None else jnp.where(sub == s, row, acc)
                if done[tile + c] is not None:
                    acc = jnp.where(lane < shift, done[tile + c][g * SUB : (g + 1) * SUB], acc)
                groups.append(acc)
            done[tile + c] = jnp.concatenate(groups, axis=0)
    for c in range(tiles):
        put_own(c, done[c])
        for q in range(2):
            put_shared(c * 2 + q, done[c][quantities - 2 + q : quantities - 1 + q])


def writers(dims, n, keep, give):
    snapshots, levels, rows, blocks, tiles, dests, per_dest = dims
    quantities = 2 * snapshots + 4
    own_rows = tiles * quantities
    dest, inner = (n // per_dest, n % per_dest) if per_dest > 1 else (n, 0)
    halves = (keep,) if give is None else (keep, give)
    half = dest if give is None else dest // 2
    shared_at = keep.shape[0] - 2 * tiles * blocks

    def put_own(c, value):
        base = (half * per_dest + inner) * own_rows + c * quantities
        if not isinstance(base, int):
            base = pl.multiple_of(base, SUB)
        at = pl.ds(base, quantities)
        if give is None:
            keep[at, :] = value
            return
        mine = lax.axis_index("lon") % 2 == dest % 2

        @pl.when(mine)
        def _():
            keep[at, :] = value

        @pl.when(jnp.logical_not(mine))
        def _():
            give[at, :] = value

    def put_shared(place, value):
        for ref in halves:
            ref[pl.ds(shared_at + place * blocks + n, 1), :] = value

    return put_own, put_shared


def inner_kernel(dims, pairs, flow, warmth, flag, floor, basin, *outs):
    rows, blocks = dims[2:4]
    keep, give = outs[:2] if pairs else (outs[0], None)
    mean_warmth, limit, depth_buf = outs[-3:]
    depth_buf[...] = (flag[...] * floor[...]).astype(jnp.float32)

    def body(n, carry):
        at = pl.multiple_of(n * SUB, SUB)
        here, north = pl.ds(at, SUB), pl.ds(at + 1, SUB)
        shallow = jnp.minimum(depth_buf[here, :], depth_buf[north, :])
        limit[here, :] = shallow

        def put_mean(k, value):
            mean_warmth[k, here, :] = value

        def get_v(t, k):
            return flow[t, k, here, :]

        def get_w(t, k):
            return 0.5 * (warmth[t, k, here, :] + warmth[t, k, north, :])

        put_own, put_shared = writers(dims, n, keep, give)
        block_sums(
            dims, n, get_v, get_w, shallow, basin[here, :], put_own, put_shared, put_mean
        )
        return carry

    lax.fori_loop(0, blocks - 1, body, 0)


def last_kernel(dims, pairs, odd_halo, even_halo, flow, warmth, flag, floor, basin, *refs):
    snapshots, levels, rows, blocks = dims[:4]
    outs = refs[len(refs) // 2 :]
    keep, give = outs[:2] if pairs else (outs[0], None)
    mean_warmth, limit = outs[-2:]
    here = slice(rows - SUB, rows)
    below = lax.broadcasted_iota(jnp.int32, (SUB, LANES), 0) < SUB - 1

    lat = lax.axis_index("lat")
    even = lat % 2 == 0
    inside = jnp.where(lat < lax.axis_size("lat") - 1, 1.0, 0.0)

    def north(block, n):
        row = jnp.where(even, even_halo[n : n + 1, :], odd_halo[n : n + 1, :]) * inside
        return jnp.where(below, pltpu.roll(block, SUB - 1, 0), row)

    depth = (flag[here, :] * floor[here, :]).astype(jnp.float32)
    edge_at = snapshots * levels
    shallow = jnp.minimum(depth, north(depth, edge_at))
    limit[here, :] = shallow

    def put_mean(k, value):
        mean_warmth[k, here, :] = value

    def get_v(t, k):
        return flow[t, k, here, :]

    def get_w(t, k):
        block = warmth[t, k, here, :]
        return 0.5 * (block + north(block, t * levels + k))

    put_own, put_shared = writers(dims, blocks - 1, keep, give)
    block_sums(
        dims, blocks - 1, get_v, get_w, shallow, basin[here, :], put_own, put_shared, put_mean
    )


def pair_kernel(dims, keep, came, *outs):
    tiles, per_dest = dims[4], dims[6]
    own_rows = per_dest * tiles * (2 * dims[0] + 4)
    chips = len(outs)
    shared = chips * own_rows
    chip = lax.axis_index("lon") // 2
    for offset, out in enumerate(outs):
        at = pl.multiple_of((chip ^ offset) * own_rows, SUB)
        out[0:own_rows, :] = keep[pl.ds(at, own_rows), :] + came[pl.ds(at, own_rows), :]
        out[own_rows:, :] = keep[shared:, :] + came[shared:, :]


def finish_kernel(dims, scaling, *refs):
    mean_warmth, limit, basin, eddy, transport = refs[-5:]
    snapshots, levels, rows, blocks, tiles, dests, per_dest = dims
    width = BASINS * SUB
    quantities = 2 * snapshots + 4
    own_rows = tiles * quantities
    sub, lane = iota(0), iota(1)
    got = refs[:-5]
    if len(got) == 1:
        got = [got[0].at[d] for d in range(got[0].shape[0])]
    mine = got[0][...]
    for part in got[1:]:
        mine = mine + part[...]
    shared = mine[per_dest * own_rows :]
    bar = []
    for c in range(tiles):
        at = c * 2 * blocks
        bar.append(shared[at : at + blocks] / jnp.maximum(shared[at + blocks : at + 2 * blocks], 1.0))
    for k in range(levels):
        level = pick_lanes(bar, k * width, width)
        for n in range(blocks):
            where = basin[n * SUB : (n + 1) * SUB, :] * SUB + sub
            row = jnp.broadcast_to(level[n : n + 1], (SUB, LANES))
            cell = jnp.take_along_axis(row, where, axis=1, mode="promise_in_bounds")
            deep = limit[n * SUB : (n + 1) * SUB, :] > float(k)
            star = mean_warmth[k, n * SUB : (n + 1) * SUB, :] - cell
            eddy[k, n * SUB : (n + 1) * SUB, :] = jnp.where(deep, star, 0.0)
    spread = jnp.minimum(lane, BASINS - 1) * SUB + sub
    for i in range(per_dest):
        terms = []
        for c in range(tiles):
            own = mine[i * own_rows + c * quantities : i * own_rows + (c + 1) * quantities]
            count = own[quantities - 1 : quantities]
            floor = jnp.maximum(count, 1.0)
            v = own[:snapshots] / floor
            w = own[snapshots : 2 * snapshots] / floor
            bar_v = jnp.sum(v, axis=0, keepdims=True) * (1.0 / snapshots)
            bar_w = jnp.sum(w, axis=0, keepdims=True) * (1.0 / snapshots)
            swing = jnp.sum((v - bar_v) * (w - bar_w), axis=0, keepdims=True) * (1.0 / snapshots)
            mean_part = count * bar_v * bar_w
            swing = count * swing
            product = own[2 * snapshots : 2 * snapshots + 1]
            cross = own[2 * snapshots + 1 : 2 * snapshots + 2]
            four = [mean_part, product - mean_part, swing, cross - swing]
            terms.append(scaling * jnp.concatenate(four + four, axis=0))
        for k in range(levels):
            level = pick_lanes(terms, k * width, width)
            for term in range(4):
                row = jnp.broadcast_to(level[term : term + 1], (SUB, LANES))
                cell = jnp.take_along_axis(row, spread, axis=1, mode="promise_in_bounds")
                transport[term, k, i * SUB : (i + 1) * SUB, :] = cell[:, :BASINS]


def neighbours(lat, lon, first):
    route = []
    for i in range(lat):
        other = i + 1 if (i - first) % 2 == 0 else i - 1
        for j in range(lon):
            if 0 <= other < lat:
                target = other * lon + j
            else:
                target = i * lon + (j ^ 1 if lon % 2 == 0 else j)
            route.append((i * lon + j, target))
    return route


def shards(flow, warmth, flag, floor, basin):
    snapshots, levels, rows, cols = flow.shape
    lon, lat = lax.axis_size("lon"), lax.axis_size("lat")
    scaling = 1.0 / math.sqrt(cols * lon)
    share = rows // lon
    blocks = rows // SUB
    per_dest = max(1, share // SUB)
    dests = blocks // per_dest
    width = BASINS * SUB
    tiles = cover(levels * width, LANES)
    quantities = 2 * snapshots + 4
    dims = (snapshots, levels, rows, blocks, tiles, dests, per_dest)
    own_rows, shared_rows = per_dest * tiles * quantities, tiles * 2 * blocks
    pairs = dests == lon and lon in (2, 4, 8)

    vmem = pl.BlockSpec(memory_space=pltpu.VMEM)
    hbm = pl.BlockSpec(memory_space=pl.ANY)
    params = pltpu.CompilerParams(vmem_limit_bytes=GRANT)

    def near(x):
        return pltpu.with_memory_space_constraint(x, pltpu.VMEM)

    def far(x):
        return pltpu.with_memory_space_constraint(x, pltpu.HBM)

    edge = pl.pallas_call(
        functools.partial(edge_kernel, dims),
        out_shape=pltpu.VMEM((snapshots * levels + 1, cols), jnp.float32),
        in_specs=[hbm] * 3,
        out_specs=vmem,
        scratch_shapes=[
            pltpu.VMEM((snapshots, levels, SUB, cols), jnp.float32),
            pltpu.VMEM((SUB, cols), jnp.int32),
            pltpu.VMEM((SUB, cols), jnp.int32),
            pltpu.SemaphoreType.DMA((snapshots + 2,)),
        ],
        compiler_params=params,
        cost_estimate=pl.CostEstimate(flops=10000000000, bytes_accessed=8 << 20, transcendentals=0),
        name="edge",
    )(far(warmth), far(flag), far(floor))
    halos = tuple(
        lax.ppermute(edge, ("lat", "lon"), neighbours(lat, lon, first)) for first in range(2)
    )

    flow, warmth, flag, floor, basin = (near(x) for x in (flow, warmth, flag, floor, basin))
    half = pltpu.VMEM((dests // 2 * own_rows + shared_rows, LANES), jnp.float32)
    full = pltpu.VMEM((dests * own_rows + shared_rows, LANES), jnp.float32)
    results = ((half, half) if pairs else (full,)) + (
        pltpu.VMEM((levels, rows, cols), jnp.float32),
        pltpu.VMEM((rows, cols), jnp.float32),
    )
    sums = pl.pallas_call(
        functools.partial(inner_kernel, dims, pairs),
        out_shape=results,
        in_specs=[vmem] * 5,
        out_specs=(vmem,) * len(results),
        scratch_shapes=[pltpu.VMEM((rows, cols), jnp.float32)],
        compiler_params=params,
        name="inner_rows",
    )(flow, warmth, flag, floor, basin)
    sums = pl.pallas_call(
        functools.partial(last_kernel, dims, pairs),
        out_shape=results,
        in_specs=[vmem] * (7 + len(results)),
        out_specs=(vmem,) * len(results),
        input_output_aliases={7 + i: i for i in range(len(results))},
        compiler_params=params,
        name="last_rows",
    )(*halos[::-1], flow, warmth, flag, floor, basin, *sums)
    mean_warmth, limit = sums[-2:]

    if pairs:
        keep, give = sums[:2]
        came = lax.ppermute(give, "lon", [(i, i ^ 1) for i in range(lon)])
        message = pltpu.VMEM((own_rows + shared_rows, LANES), jnp.float32)
        chips = lon // 2
        messages = pl.pallas_call(
            functools.partial(pair_kernel, dims),
            out_shape=(message,) * chips,
            in_specs=[vmem, vmem],
            out_specs=(vmem,) * chips,
            compiler_params=params,
            name="pair_sums",
        )(keep, came)
        got = messages[:1] + tuple(
            lax.ppermute(messages[m], "lon", [(i, i ^ (2 * m)) for i in range(lon)])
            for m in reversed(range(1, chips))
        )
    else:
        own, shared = sums[0][: dests * own_rows], sums[0][dests * own_rows :]
        sent = jnp.concatenate(
            [own.reshape(dests, own_rows, LANES), jnp.broadcast_to(shared, (dests, shared_rows, LANES))],
            axis=1,
        )
        if dests != lon:
            sent = jnp.repeat(sent, lon // dests, axis=0, total_repeat_length=lon)
        got = (lax.all_to_all(sent, "lon", 0, 0),)

    eddy, transport = pl.pallas_call(
        functools.partial(finish_kernel, dims, scaling),
        out_shape=(
            jax.ShapeDtypeStruct((levels, rows, cols), jnp.float32),
            jax.ShapeDtypeStruct((4, levels, per_dest * SUB, BASINS), jnp.float32),
        ),
        in_specs=[vmem] * (len(got) + 3),
        out_specs=(vmem, vmem),
        compiler_params=params,
        name="finish",
    )(*got, mean_warmth, limit, basin)
    if dests != lon:
        first = lax.axis_index("lon") * share % SUB
        transport = lax.dynamic_slice_in_dim(transport, first, share, 2)
    return eddy, jnp.transpose(transport, (0, 3, 1, 2))


def solution(mesh):
    return jax.shard_map(
        shards,
        mesh=mesh,
        in_specs=(
            P(None, None, "lat", "lon"),
            P(None, None, "lat", "lon"),
            P("lat", "lon"),
            P("lat", "lon"),
            P("lat", "lon"),
        ),
        out_specs=(P(None, "lat", "lon"), P(None, None, None, ("lat", "lon"))),
        check_vma=False,
    )
```

```python
import functools
import math

import jax
import jax.numpy as jnp
from jax import lax
from jax.experimental import pallas as pl
from jax.experimental.pallas import tpu as pltpu
from jax.sharding import PartitionSpec as P

BASINS = 10
SUB = 8
LANES = 128
CUT = 80
GRANT = 16 * 1024 * 1024


def cover(total, unit):
    return -(-total // unit)


def iota(axis):
    return lax.broadcasted_iota(jnp.int32, (SUB, LANES), axis)


def pick_lanes(tiles, start, width):
    first, shift = divmod(start, LANES)
    if shift == 0:
        return tiles[first]
    left = pltpu.roll(tiles[first], LANES - shift, 1)
    if shift + width <= LANES:
        return left
    right = pltpu.roll(tiles[first + 1], LANES - shift, 1)
    return jnp.where(lax.broadcasted_iota(jnp.int32, left.shape, 1) < LANES - shift, left, right)


def edge_kernel(dims, warmth, flag, floor, edge, rows_buf, flag_buf, floor_buf, sem):
    snapshots, levels = dims[:2]
    first = slice(0, SUB)
    copies = [
        pltpu.make_async_copy(flag.at[first, :], flag_buf, sem.at[snapshots]),
        pltpu.make_async_copy(floor.at[first, :], floor_buf, sem.at[snapshots + 1]),
    ] + [
        pltpu.make_async_copy(warmth.at[t, :, first, :], rows_buf.at[t], sem.at[t])
        for t in range(snapshots)
    ]
    for copy in copies:
        copy.start()
    for copy in copies:
        copy.wait()
    depth = (flag_buf[0:1, :] * floor_buf[0:1, :]).astype(jnp.float32)
    edge[snapshots * levels : snapshots * levels + 1, :] = depth
    for t in range(snapshots):
        for k in range(levels):
            edge[t * levels + k : t * levels + k + 1, :] = rows_buf[t, k, 0:1, :]


def prepare(dims, rows_of, room):
    snapshots, levels = dims[:2]
    get_v, get_w, put_mean = rows_of
    for k in range(levels):
        v = [get_v(t, k) for t in range(snapshots)]
        w = [get_w(t, k) for t in range(snapshots)]
        mv = sum(v[1:], v[0]) * (1.0 / snapshots)
        mw = sum(w[1:], w[0]) * (1.0 / snapshots)
        cross = sum((a - mv) * (b - mw) for a, b in zip(v, w)) * (1.0 / snapshots)
        put_mean(k, mw)
        for at, value in enumerate(w + [mv * mw, cross, mw]):
            room[k, at] = value


def multiply(dims, group, get_v, room, shallow, label):
    snapshots = dims[0]
    width = BASINS * SUB
    nothing = jnp.zeros((SUB, LANES), jnp.float32)

    def level_data(k):
        v = [get_v(t, k) for t in range(snapshots)]
        rest = [room[k, at] for at in range(snapshots + 3)]
        return jnp.concatenate(v + rest + [jnp.ones((SUB, LANES), jnp.float32)], axis=0)

    def level_hot(k):
        masked = jnp.where(shallow > float(k), label, -1)
        return [jnp.where(masked == b, 1.0, 0.0) for b in range(BASINS)]

    data = jnp.concatenate([level_data(k) for k in group], axis=1)
    columns = []
    for k in group:
        column = [nothing] * (group[0] * width % LANES // SUB)
        for other in group:
            column += level_hot(k) if other == k else [nothing] * BASINS
        columns.append(jnp.concatenate(column, axis=0))
    hot = jnp.concatenate(columns, axis=1).astype(jnp.bfloat16)
    exact, height = 2 * snapshots * SUB, data.shape[0]
    cuts = list(range(0, exact, CUT)) + [exact, height]
    parts, spans = [], []
    for at, end in zip(cuts, cuts[1:]):
        rest = data[at:end]
        count = 2 if at < exact else 3
        for piece in range(count):
            parts.append(rest.astype(jnp.bfloat16))
            if piece < count - 1:
                rest = rest - parts[-1].astype(jnp.float32)
        spans.append((end - at, count))
    dots = lax.dot_general(
        jnp.concatenate(parts, axis=0),
        hot,
        (((1,), (1,)), ((), ())),
        preferred_element_type=jnp.float32,
    )
    sums, at = [], 0
    for size, count in spans:
        x = dots[at : at + size]
        for piece in range(1, count):
            x = x + dots[at + piece * size : at + (piece + 1) * size]
        sums.append(x)
        at += size * count
    total = jnp.concatenate(sums, axis=0)
    spare = -total.shape[1] % LANES
    if spare:
        total = jnp.concatenate([total, jnp.zeros((total.shape[0], spare), jnp.float32)], axis=1)
    return total


def extract(dims, group, total, done):
    quantities = 2 * dims[0] + 4
    sub, lane = iota(0), iota(1)
    diagonal = lane % SUB
    tile, shift = divmod(group[0] * BASINS * SUB, LANES)
    for c in range(total.shape[1] // LANES):
        groups = []
        for g in range(quantities // SUB):
            acc = None
            for s in range(SUB):
                q = g * SUB + s
                row = jnp.take_along_axis(
                    total[q * SUB : (q + 1) * SUB, c * LANES : (c + 1) * LANES],
                    diagonal,
                    axis=0,
                    mode="promise_in_bounds",
                )
                acc = row if acc is None else jnp.where(sub == s, row, acc)
            if done[tile + c] is not None:
                acc = jnp.where(lane < shift, done[tile + c][g * SUB : (g + 1) * SUB], acc)
            groups.append(acc)
        done[tile + c] = jnp.concatenate(groups, axis=0)


def level_groups(dims):
    return [tuple(range(k, min(k + 2, dims[1]))) for k in range(0, dims[1], 2)]


def store_block(dims, n, done, keep, give):
    quantities = 2 * dims[0] + 4
    put_own, put_shared = writers(dims, n, keep, give)
    for c in range(dims[4]):
        put_own(c, done[c])
        for q in range(2):
            put_shared(c * 2 + q, done[c][quantities - 2 + q : quantities - 1 + q])


def writers(dims, n, keep, give):
    snapshots, levels, rows, blocks, tiles, dests, per_dest = dims
    quantities = 2 * snapshots + 4
    own_rows = tiles * quantities
    dest, inner = (n // per_dest, n % per_dest) if per_dest > 1 else (n, 0)
    halves = (keep,) if give is None else (keep, give)
    half = dest if give is None else dest // 2
    shared_at = keep.shape[0] - 2 * tiles * blocks

    def put_own(c, value):
        base = (half * per_dest + inner) * own_rows + c * quantities
        if not isinstance(base, int):
            base = pl.multiple_of(base, SUB)
        at = pl.ds(base, quantities)
        if give is None:
            keep[at, :] = value
            return
        mine = lax.axis_index("lon") % 2 == dest % 2

        @pl.when(mine)
        def _():
            keep[at, :] = value

        @pl.when(jnp.logical_not(mine))
        def _():
            give[at, :] = value

    def put_shared(place, value):
        for ref in halves:
            ref[pl.ds(shared_at + place * blocks + n, 1), :] = value

    return put_own, put_shared


def inner_kernel(dims, pairs, flow, warmth, flag, floor, basin, *refs):
    blocks, tiles = dims[3:5]
    outs, room = refs[:-1], refs[-1]
    keep, give = outs[:2] if pairs else (outs[0], None)
    mean_warmth, limit = outs[-2:]

    def span(n):
        at = n * SUB if isinstance(n, int) else pl.multiple_of(n * SUB, SUB)
        return pl.ds(at, SUB), pl.ds(at + 1, SUB)

    def rows_of(n):
        here, north = span(n)

        def put_mean(k, value):
            mean_warmth[k, here, :] = value

        def get_v(t, k):
            return flow[t, k, here, :]

        def get_w(t, k):
            return 0.5 * (warmth[t, k, here, :] + warmth[t, k, north, :])

        return get_v, get_w, put_mean

    def several(ns):
        work = []
        for n in ns:
            here, north = span(n)
            depth = (flag[here, :] * floor[here, :]).astype(jnp.float32)
            upper = (flag[north, :] * floor[north, :]).astype(jnp.float32)
            shallow = jnp.minimum(depth, upper)
            limit[here, :] = shallow
            work.append((n, rows_of(n), shallow, basin[here, :], [None] * tiles))
        totals = []
        rooms = [room.at[i] for i in range(7)]
        for (n, rows, shallow, label, done), r in zip(work, rooms):
            prepare(dims, rows, r)
            for group in level_groups(dims):
                totals.append((group, done, multiply(dims, group, rows[0], r, shallow, label)))
        for group, done, total in totals:
            extract(dims, group, total, done)

        for n, _, _, _, done in work:
            store_block(dims, n, done, keep, give)

    def body(i, carry):
        several([i * 7 + j for j in range(7)])
        return carry

    lax.fori_loop(0, (blocks - 1) // 7, body, 0)
    rest = (blocks - 1) % 7
    if rest:
        several(list(range(blocks - 1 - rest, blocks - 1)))


def last_kernel(dims, pairs, odd_halo, even_halo, flow, warmth, flag, floor, basin, *refs):
    snapshots, levels, rows, blocks = dims[:4]
    refs, room = refs[:-1], refs[-1]
    outs = refs[len(refs) // 2 :]
    keep, give = outs[:2] if pairs else (outs[0], None)
    mean_warmth, limit = outs[-2:]
    here = slice(rows - SUB, rows)
    below = lax.broadcasted_iota(jnp.int32, (SUB, LANES), 0) < SUB - 1

    lat = lax.axis_index("lat")
    even = lat % 2 == 0
    inside = jnp.where(lat < lax.axis_size("lat") - 1, 1.0, 0.0)

    def north(block, n):
        row = jnp.where(even, even_halo[n : n + 1, :], odd_halo[n : n + 1, :]) * inside
        return jnp.where(below, pltpu.roll(block, SUB - 1, 0), row)

    depth = (flag[here, :] * floor[here, :]).astype(jnp.float32)
    edge_at = snapshots * levels
    shallow = jnp.minimum(depth, north(depth, edge_at))
    limit[here, :] = shallow

    def put_mean(k, value):
        mean_warmth[k, here, :] = value

    def get_v(t, k):
        return flow[t, k, here, :]

    def get_w(t, k):
        block = warmth[t, k, here, :]
        return 0.5 * (block + north(block, t * levels + k))

    room = room.at[0]
    prepare(dims, (get_v, get_w, put_mean), room)
    done = [None] * dims[4]
    for group in level_groups(dims):
        total = multiply(dims, group, get_v, room, shallow, basin[here, :])
        extract(dims, group, total, done)
    store_block(dims, blocks - 1, done, keep, give)


def pair_kernel(dims, keep, came, *outs):
    tiles, per_dest = dims[4], dims[6]
    own_rows = per_dest * tiles * (2 * dims[0] + 4)
    chips = len(outs)
    shared = chips * own_rows
    chip = lax.axis_index("lon") // 2
    for offset, out in enumerate(outs):
        at = pl.multiple_of((chip ^ offset) * own_rows, SUB)
        out[0:own_rows, :] = keep[pl.ds(at, own_rows), :] + came[pl.ds(at, own_rows), :]
        out[own_rows:, :] = keep[shared:, :] + came[shared:, :]


def finish_kernel(dims, scaling, *refs):
    mean_warmth, limit, basin, eddy, transport = refs[-5:]
    snapshots, levels, rows, blocks, tiles, dests, per_dest = dims
    width = BASINS * SUB
    quantities = 2 * snapshots + 4
    own_rows = tiles * quantities
    sub, lane = iota(0), iota(1)
    got = refs[:-5]
    if len(got) == 1:
        got = [got[0].at[d] for d in range(got[0].shape[0])]
    mine = got[0][...]
    for part in got[1:]:
        mine = mine + part[...]
    shared = mine[per_dest * own_rows :]
    bar = []
    for c in range(tiles):
        at = c * 2 * blocks
        bar.append(shared[at : at + blocks] / jnp.maximum(shared[at + blocks : at + 2 * blocks], 1.0))
    for k in range(levels):
        level = pick_lanes(bar, k * width, width)
        for n in range(blocks):
            where = basin[n * SUB : (n + 1) * SUB, :] * SUB + sub
            row = jnp.broadcast_to(level[n : n + 1], (SUB, LANES))
            cell = jnp.take_along_axis(row, where, axis=1, mode="promise_in_bounds")
            deep = limit[n * SUB : (n + 1) * SUB, :] > float(k)
            star = mean_warmth[k, n * SUB : (n + 1) * SUB, :] - cell
            eddy[k, n * SUB : (n + 1) * SUB, :] = jnp.where(deep, star, 0.0)
    spread = jnp.minimum(lane, BASINS - 1) * SUB + sub
    for i in range(per_dest):
        terms = []
        for c in range(tiles):
            own = mine[i * own_rows + c * quantities : i * own_rows + (c + 1) * quantities]
            count = own[quantities - 1 : quantities]
            floor = jnp.maximum(count, 1.0)
            v = own[:snapshots] / floor
            w = own[snapshots : 2 * snapshots] / floor
            bar_v = jnp.sum(v, axis=0, keepdims=True) * (1.0 / snapshots)
            bar_w = jnp.sum(w, axis=0, keepdims=True) * (1.0 / snapshots)
            swing = jnp.sum((v - bar_v) * (w - bar_w), axis=0, keepdims=True) * (1.0 / snapshots)
            mean_part = count * bar_v * bar_w
            swing = count * swing
            product = own[2 * snapshots : 2 * snapshots + 1]
            cross = own[2 * snapshots + 1 : 2 * snapshots + 2]
            four = [mean_part, product - mean_part, swing, cross - swing]
            terms.append(scaling * jnp.concatenate(four + four, axis=0))
        for k in range(levels):
            level = pick_lanes(terms, k * width, width)
            for term in range(4):
                row = jnp.broadcast_to(level[term : term + 1], (SUB, LANES))
                cell = jnp.take_along_axis(row, spread, axis=1, mode="promise_in_bounds")
                transport[term, k, i * SUB : (i + 1) * SUB, :] = cell[:, :BASINS]


def neighbours(lat, lon, first):
    route = []
    for i in range(lat):
        other = i + 1 if (i - first) % 2 == 0 else i - 1
        for j in range(lon):
            if 0 <= other < lat:
                target = other * lon + j
            else:
                target = i * lon + (j ^ 1 if lon % 2 == 0 else j)
            route.append((i * lon + j, target))
    return route


def shards(flow, warmth, flag, floor, basin):
    snapshots, levels, rows, cols = flow.shape
    lon, lat = lax.axis_size("lon"), lax.axis_size("lat")
    scaling = 1.0 / math.sqrt(cols * lon)
    share = rows // lon
    blocks = rows // SUB
    per_dest = max(1, share // SUB)
    dests = blocks // per_dest
    width = BASINS * SUB
    tiles = cover(levels * width, LANES)
    quantities = 2 * snapshots + 4
    dims = (snapshots, levels, rows, blocks, tiles, dests, per_dest)
    own_rows, shared_rows = per_dest * tiles * quantities, tiles * 2 * blocks
    pairs = dests == lon and lon in (2, 4, 8)

    vmem = pl.BlockSpec(memory_space=pltpu.VMEM)
    hbm = pl.BlockSpec(memory_space=pl.ANY)
    params = pltpu.CompilerParams(vmem_limit_bytes=GRANT)

    def near(x):
        return pltpu.with_memory_space_constraint(x, pltpu.VMEM)

    def far(x):
        return pltpu.with_memory_space_constraint(x, pltpu.HBM)

    edge = pl.pallas_call(
        functools.partial(edge_kernel, dims),
        out_shape=pltpu.VMEM((snapshots * levels + 1, cols), jnp.float32),
        in_specs=[hbm] * 3,
        out_specs=vmem,
        scratch_shapes=[
            pltpu.VMEM((snapshots, levels, SUB, cols), jnp.float32),
            pltpu.VMEM((SUB, cols), jnp.int32),
            pltpu.VMEM((SUB, cols), jnp.int32),
            pltpu.SemaphoreType.DMA((snapshots + 2,)),
        ],
        compiler_params=params,
        cost_estimate=pl.CostEstimate(flops=10000000000, bytes_accessed=8 << 20, transcendentals=0),
        name="edge",
    )(far(warmth), far(flag), far(floor))
    halos = tuple(
        lax.ppermute(edge, ("lat", "lon"), neighbours(lat, lon, first)) for first in range(2)
    )

    flow, warmth, flag, floor, basin = (near(x) for x in (flow, warmth, flag, floor, basin))
    half = pltpu.VMEM((dests // 2 * own_rows + shared_rows, LANES), jnp.float32)
    full = pltpu.VMEM((dests * own_rows + shared_rows, LANES), jnp.float32)
    results = ((half, half) if pairs else (full,)) + (
        pltpu.VMEM((levels, rows, cols), jnp.float32),
        pltpu.VMEM((rows, cols), jnp.float32),
    )
    room = pltpu.VMEM((7, levels, snapshots + 3, SUB, cols), jnp.float32)
    sums = pl.pallas_call(
        functools.partial(inner_kernel, dims, pairs),
        out_shape=results,
        in_specs=[vmem] * 5,
        out_specs=(vmem,) * len(results),
        scratch_shapes=[room],
        compiler_params=params,
        name="inner_rows",
    )(flow, warmth, flag, floor, basin)
    sums = pl.pallas_call(
        functools.partial(last_kernel, dims, pairs),
        out_shape=results,
        in_specs=[vmem] * (7 + len(results)),
        out_specs=(vmem,) * len(results),
        input_output_aliases={7 + i: i for i in range(len(results))},
        scratch_shapes=[room],
        compiler_params=params,
        name="last_rows",
    )(*halos[::-1], flow, warmth, flag, floor, basin, *sums)
    mean_warmth, limit = sums[-2:]

    if pairs:
        keep, give = sums[:2]
        came = lax.ppermute(give, "lon", [(i, i ^ 1) for i in range(lon)])
        message = pltpu.VMEM((own_rows + shared_rows, LANES), jnp.float32)
        chips = lon // 2
        messages = pl.pallas_call(
            functools.partial(pair_kernel, dims),
            out_shape=(message,) * chips,
            in_specs=[vmem, vmem],
            out_specs=(vmem,) * chips,
            compiler_params=params,
            name="pair_sums",
        )(keep, came)
        got = messages[:1] + tuple(
            lax.ppermute(messages[m], "lon", [(i, i ^ (2 * m)) for i in range(lon)])
            for m in reversed(range(1, chips))
        )
    else:
        own, shared = sums[0][: dests * own_rows], sums[0][dests * own_rows :]
        sent = jnp.concatenate(
            [own.reshape(dests, own_rows, LANES), jnp.broadcast_to(shared, (dests, shared_rows, LANES))],
            axis=1,
        )
        if dests != lon:
            sent = jnp.repeat(sent, lon // dests, axis=0, total_repeat_length=lon)
        got = (lax.all_to_all(sent, "lon", 0, 0),)

    eddy, transport = pl.pallas_call(
        functools.partial(finish_kernel, dims, scaling),
        out_shape=(
            jax.ShapeDtypeStruct((levels, rows, cols), jnp.float32),
            jax.ShapeDtypeStruct((4, levels, per_dest * SUB, BASINS), jnp.float32),
        ),
        in_specs=[vmem] * (len(got) + 3),
        out_specs=(vmem, vmem),
        compiler_params=params,
        name="finish",
    )(*got, mean_warmth, limit, basin)
    if dests != lon:
        first = lax.axis_index("lon") * share % SUB
        transport = lax.dynamic_slice_in_dim(transport, first, share, 2)
    return eddy, jnp.transpose(transport, (0, 3, 1, 2))


def solution(mesh):
    return jax.shard_map(
        shards,
        mesh=mesh,
        in_specs=(
            P(None, None, "lat", "lon"),
            P(None, None, "lat", "lon"),
            P("lat", "lon"),
            P("lat", "lon"),
            P("lat", "lon"),
        ),
        out_specs=(P(None, "lat", "lon"), P(None, None, None, ("lat", "lon"))),
        check_vma=False,
    )
```

```python
import functools
import math

import jax
import jax.numpy as jnp
from jax import lax
from jax.experimental import pallas as pl
from jax.experimental.pallas import tpu as pltpu
from jax.sharding import PartitionSpec as P

BASINS = 10
SUB = 8
LANES = 128
CUT = 80
GRANT = 16 * 1024 * 1024


def cover(total, unit):
    return -(-total // unit)


def iota(axis):
    return lax.broadcasted_iota(jnp.int32, (SUB, LANES), axis)


def pick_lanes(tiles, start, width):
    first, shift = divmod(start, LANES)
    if shift == 0:
        return tiles[first]
    left = pltpu.roll(tiles[first], LANES - shift, 1)
    if shift + width <= LANES:
        return left
    right = pltpu.roll(tiles[first + 1], LANES - shift, 1)
    return jnp.where(lax.broadcasted_iota(jnp.int32, left.shape, 1) < LANES - shift, left, right)


def edge_kernel(dims, warmth, flag, floor, edge, rows_buf, flag_buf, floor_buf, sem):
    snapshots, levels = dims[:2]
    first = slice(0, SUB)
    copies = [
        pltpu.make_async_copy(flag.at[first, :], flag_buf, sem.at[snapshots]),
        pltpu.make_async_copy(floor.at[first, :], floor_buf, sem.at[snapshots + 1]),
    ] + [
        pltpu.make_async_copy(warmth.at[t, :, first, :], rows_buf.at[t], sem.at[t])
        for t in range(snapshots)
    ]
    for copy in copies:
        copy.start()
    for copy in copies:
        copy.wait()
    depth = (flag_buf[0:1, :] * floor_buf[0:1, :]).astype(jnp.float32)
    edge[snapshots * levels : snapshots * levels + 1, :] = depth
    for t in range(snapshots):
        for k in range(levels):
            edge[t * levels + k : t * levels + k + 1, :] = rows_buf[t, k, 0:1, :]


def prepare(dims, rows_of, room):
    snapshots, levels = dims[:2]
    get_v, get_w, put_mean = rows_of
    for k in range(levels):
        v = [get_v(t, k) for t in range(snapshots)]
        w = [get_w(t, k) for t in range(snapshots)]
        mv = sum(v[1:], v[0]) * (1.0 / snapshots)
        mw = sum(w[1:], w[0]) * (1.0 / snapshots)
        cross = sum((a - mv) * (b - mw) for a, b in zip(v, w)) * (1.0 / snapshots)
        put_mean(k, mw)
        for at, value in enumerate(w + [mv * mw, cross, mw]):
            room[k, at] = value


def multiply(dims, group, get_v, room, shallow, label):
    snapshots = dims[0]
    width = BASINS * SUB
    nothing = jnp.zeros((SUB, LANES), jnp.float32)

    def level_data(k):
        v = [get_v(t, k) for t in range(snapshots)]
        rest = [room[k, at] for at in range(snapshots + 3)]
        return jnp.concatenate(v + rest + [jnp.ones((SUB, LANES), jnp.float32)], axis=0)

    def level_hot(k):
        masked = jnp.where(shallow > float(k), label, -1)
        return [jnp.where(masked == b, 1.0, 0.0) for b in range(BASINS)]

    data = jnp.concatenate([level_data(k) for k in group], axis=1)
    columns = []
    for k in group:
        column = [nothing] * (group[0] * width % LANES // SUB)
        for other in group:
            column += level_hot(k) if other == k else [nothing] * BASINS
        columns.append(jnp.concatenate(column, axis=0))
    hot = jnp.concatenate(columns, axis=1).astype(jnp.bfloat16)
    exact, height = 2 * snapshots * SUB, data.shape[0]
    cuts = list(range(0, exact, CUT)) + [exact, height]
    parts, spans = [], []
    for at, end in zip(cuts, cuts[1:]):
        rest = data[at:end]
        count = 2 if at < exact else 3
        for piece in range(count):
            parts.append(rest.astype(jnp.bfloat16))
            if piece < count - 1:
                rest = rest - parts[-1].astype(jnp.float32)
        spans.append((end - at, count))
    dots = lax.dot_general(
        jnp.concatenate(parts, axis=0),
        hot,
        (((1,), (1,)), ((), ())),
        preferred_element_type=jnp.float32,
    )
    sums, at = [], 0
    for size, count in spans:
        x = dots[at : at + size]
        for piece in range(1, count):
            x = x + dots[at + piece * size : at + (piece + 1) * size]
        sums.append(x)
        at += size * count
    total = jnp.concatenate(sums, axis=0)
    spare = -total.shape[1] % LANES
    if spare:
        total = jnp.concatenate([total, jnp.zeros((total.shape[0], spare), jnp.float32)], axis=1)
    return total


def extract(dims, group, total, done):
    quantities = 2 * dims[0] + 4
    sub, lane = iota(0), iota(1)
    diagonal = lane % SUB
    tile, shift = divmod(group[0] * BASINS * SUB, LANES)
    for c in range(total.shape[1] // LANES):
        groups = []
        for g in range(quantities // SUB):
            acc = None
            for s in range(SUB):
                q = g * SUB + s
                row = jnp.take_along_axis(
                    total[q * SUB : (q + 1) * SUB, c * LANES : (c + 1) * LANES],
                    diagonal,
                    axis=0,
                    mode="promise_in_bounds",
                )
                acc = row if acc is None else jnp.where(sub == s, row, acc)
            if done[tile + c] is not None:
                acc = jnp.where(lane < shift, done[tile + c][g * SUB : (g + 1) * SUB], acc)
            groups.append(acc)
        done[tile + c] = jnp.concatenate(groups, axis=0)


def level_groups(dims):
    return [tuple(range(k, min(k + 2, dims[1]))) for k in range(0, dims[1], 2)]


def store_block(dims, n, done, keep, give):
    quantities = 2 * dims[0] + 4
    put_own, put_shared = writers(dims, n, keep, give)
    for c in range(dims[4]):
        put_own(c, done[c])
        for q in range(2):
            put_shared(c * 2 + q, done[c][quantities - 2 + q : quantities - 1 + q])


def writers(dims, n, keep, give):
    snapshots, levels, rows, blocks, tiles, dests, per_dest = dims
    quantities = 2 * snapshots + 4
    own_rows = tiles * quantities
    dest, inner = (n // per_dest, n % per_dest) if per_dest > 1 else (n, 0)
    halves = (keep,) if give is None else (keep, give)
    half = dest if give is None else dest // 2
    shared_at = keep.shape[0] - 2 * tiles * blocks

    def put_own(c, value):
        base = (half * per_dest + inner) * own_rows + c * quantities
        if not isinstance(base, int):
            base = pl.multiple_of(base, SUB)
        at = pl.ds(base, quantities)
        if give is None:
            keep[at, :] = value
            return
        me = lax.axis_index("lon")
        mine = (me % 2 == dest % 2) == (me // 2 == dest // 2)

        @pl.when(mine)
        def _():
            keep[at, :] = value

        @pl.when(jnp.logical_not(mine))
        def _():
            give[at, :] = value

    def put_shared(place, value):
        for ref in halves:
            ref[pl.ds(shared_at + place * blocks + n, 1), :] = value

    return put_own, put_shared


def inner_kernel(dims, pairs, flow, warmth, flag, floor, basin, *refs):
    blocks, tiles = dims[3:5]
    outs, room = refs[:-1], refs[-1]
    keep, give = outs[:2] if pairs else (outs[0], None)
    mean_warmth, limit = outs[-2:]

    def span(n):
        at = n * SUB if isinstance(n, int) else pl.multiple_of(n * SUB, SUB)
        return pl.ds(at, SUB), pl.ds(at + 1, SUB)

    def rows_of(n):
        here, north = span(n)

        def put_mean(k, value):
            mean_warmth[k, here, :] = value

        def get_v(t, k):
            return flow[t, k, here, :]

        def get_w(t, k):
            return 0.5 * (warmth[t, k, here, :] + warmth[t, k, north, :])

        return get_v, get_w, put_mean

    def several(ns):
        work = []
        for n in ns:
            here, north = span(n)
            depth = (flag[here, :] * floor[here, :]).astype(jnp.float32)
            upper = (flag[north, :] * floor[north, :]).astype(jnp.float32)
            shallow = jnp.minimum(depth, upper)
            limit[here, :] = shallow
            work.append((n, rows_of(n), shallow, basin[here, :], [None] * tiles))
        totals = []
        rooms = [room.at[i] for i in range(7)]
        for (n, rows, shallow, label, done), r in zip(work, rooms):
            prepare(dims, rows, r)
        for group in level_groups(dims):
            for (n, rows, shallow, label, done), r in zip(work, rooms):
                totals.append((group, done, multiply(dims, group, rows[0], r, shallow, label)))
        for group, done, total in totals:
            extract(dims, group, total, done)

        for n, _, _, _, done in work:
            store_block(dims, n, done, keep, give)

    def body(i, carry):
        several([i * 7 + j for j in range(7)])
        return carry

    lax.fori_loop(0, (blocks - 1) // 7, body, 0)
    rest = (blocks - 1) % 7
    if rest:
        several(list(range(blocks - 1 - rest, blocks - 1)))


def last_kernel(dims, pairs, odd_halo, even_halo, flow, warmth, flag, floor, basin, *refs):
    snapshots, levels, rows, blocks = dims[:4]
    refs, room = refs[:-1], refs[-1]
    outs = refs[len(refs) // 2 :]
    keep, give = outs[:2] if pairs else (outs[0], None)
    mean_warmth, limit = outs[-2:]
    here = slice(rows - SUB, rows)
    below = lax.broadcasted_iota(jnp.int32, (SUB, LANES), 0) < SUB - 1

    lat = lax.axis_index("lat")
    even = lat % 2 == 0
    inside = jnp.where(lat < lax.axis_size("lat") - 1, 1.0, 0.0)

    def north(block, n):
        row = jnp.where(even, even_halo[n : n + 1, :], odd_halo[n : n + 1, :]) * inside
        return jnp.where(below, pltpu.roll(block, SUB - 1, 0), row)

    depth = (flag[here, :] * floor[here, :]).astype(jnp.float32)
    edge_at = snapshots * levels
    shallow = jnp.minimum(depth, north(depth, edge_at))
    limit[here, :] = shallow

    def put_mean(k, value):
        mean_warmth[k, here, :] = value

    def get_v(t, k):
        return flow[t, k, here, :]

    def get_w(t, k):
        block = warmth[t, k, here, :]
        return 0.5 * (block + north(block, t * levels + k))

    room = room.at[0]
    prepare(dims, (get_v, get_w, put_mean), room)
    done = [None] * dims[4]
    for group in level_groups(dims):
        total = multiply(dims, group, get_v, room, shallow, basin[here, :])
        extract(dims, group, total, done)
    store_block(dims, blocks - 1, done, keep, give)


def pair_kernel(dims, keep, came, *outs):
    tiles, per_dest = dims[4], dims[6]
    own_rows = per_dest * tiles * (2 * dims[0] + 4)
    chips = len(outs)
    shared = chips * own_rows
    chip = lax.axis_index("lon") // 2
    for offset, out in enumerate(outs):
        at = pl.multiple_of((chip ^ offset) * own_rows, SUB)
        out[0:own_rows, :] = keep[pl.ds(at, own_rows), :] + came[pl.ds(at, own_rows), :]
        out[own_rows:, :] = keep[shared:, :] + came[shared:, :]


def finish_kernel(dims, scaling, *refs):
    mean_warmth, limit, basin, eddy, transport = refs[-5:]
    snapshots, levels, rows, blocks, tiles, dests, per_dest = dims
    width = BASINS * SUB
    quantities = 2 * snapshots + 4
    own_rows = tiles * quantities
    sub, lane = iota(0), iota(1)
    got = refs[:-5]
    if len(got) == 1:
        got = [got[0].at[d] for d in range(got[0].shape[0])]
    mine = got[0][...]
    for part in got[1:]:
        mine = mine + part[...]
    shared = mine[per_dest * own_rows :]
    bar = []
    for c in range(tiles):
        at = c * 2 * blocks
        bar.append(shared[at : at + blocks] / jnp.maximum(shared[at + blocks : at + 2 * blocks], 1.0))
    for k in range(levels):
        level = pick_lanes(bar, k * width, width)
        for n in range(blocks):
            where = basin[n * SUB : (n + 1) * SUB, :] * SUB + sub
            row = jnp.broadcast_to(level[n : n + 1], (SUB, LANES))
            cell = jnp.take_along_axis(row, where, axis=1, mode="promise_in_bounds")
            deep = limit[n * SUB : (n + 1) * SUB, :] > float(k)
            star = mean_warmth[k, n * SUB : (n + 1) * SUB, :] - cell
            eddy[k, n * SUB : (n + 1) * SUB, :] = jnp.where(deep, star, 0.0)
    spread = jnp.minimum(lane, BASINS - 1) * SUB + sub
    for i in range(per_dest):
        terms = []
        for c in range(tiles):
            own = mine[i * own_rows + c * quantities : i * own_rows + (c + 1) * quantities]
            count = own[quantities - 1 : quantities]
            floor = jnp.maximum(count, 1.0)
            v = own[:snapshots] / floor
            w = own[snapshots : 2 * snapshots] / floor
            bar_v = jnp.sum(v, axis=0, keepdims=True) * (1.0 / snapshots)
            bar_w = jnp.sum(w, axis=0, keepdims=True) * (1.0 / snapshots)
            swing = jnp.sum((v - bar_v) * (w - bar_w), axis=0, keepdims=True) * (1.0 / snapshots)
            mean_part = count * bar_v * bar_w
            swing = count * swing
            product = own[2 * snapshots : 2 * snapshots + 1]
            cross = own[2 * snapshots + 1 : 2 * snapshots + 2]
            four = [mean_part, product - mean_part, swing, cross - swing]
            terms.append(scaling * jnp.concatenate(four + four, axis=0))
        for k in range(levels):
            level = pick_lanes(terms, k * width, width)
            for term in range(4):
                row = jnp.broadcast_to(level[term : term + 1], (SUB, LANES))
                cell = jnp.take_along_axis(row, spread, axis=1, mode="promise_in_bounds")
                transport[term, k, i * SUB : (i + 1) * SUB, :] = cell[:, :BASINS]


def neighbours(lat, lon, first):
    route = []
    for i in range(lat):
        other = i + 1 if (i - first) % 2 == 0 else i - 1
        for j in range(lon):
            across = j ^ 1 if lon % 2 == 0 else j
            if not 0 <= other < lat:
                target = i * lon + across
            elif other < i:
                target = other * lon + j
            else:
                target = other * lon + across
            route.append((i * lon + j, target))
    return route


def shards(flow, warmth, flag, floor, basin):
    snapshots, levels, rows, cols = flow.shape
    lon, lat = lax.axis_size("lon"), lax.axis_size("lat")
    scaling = 1.0 / math.sqrt(cols * lon)
    share = rows // lon
    blocks = rows // SUB
    per_dest = max(1, share // SUB)
    dests = blocks // per_dest
    width = BASINS * SUB
    tiles = cover(levels * width, LANES)
    quantities = 2 * snapshots + 4
    dims = (snapshots, levels, rows, blocks, tiles, dests, per_dest)
    own_rows, shared_rows = per_dest * tiles * quantities, tiles * 2 * blocks
    pairs = dests == lon and lon in (2, 4, 8)

    vmem = pl.BlockSpec(memory_space=pltpu.VMEM)
    hbm = pl.BlockSpec(memory_space=pl.ANY)
    params = pltpu.CompilerParams(vmem_limit_bytes=GRANT)

    def near(x):
        return pltpu.with_memory_space_constraint(x, pltpu.VMEM)

    def far(x):
        return pltpu.with_memory_space_constraint(x, pltpu.HBM)

    edge = pl.pallas_call(
        functools.partial(edge_kernel, dims),
        out_shape=pltpu.VMEM((snapshots * levels + 1, cols), jnp.float32),
        in_specs=[hbm] * 3,
        out_specs=vmem,
        scratch_shapes=[
            pltpu.VMEM((snapshots, levels, SUB, cols), jnp.float32),
            pltpu.VMEM((SUB, cols), jnp.int32),
            pltpu.VMEM((SUB, cols), jnp.int32),
            pltpu.SemaphoreType.DMA((snapshots + 2,)),
        ],
        compiler_params=params,
        cost_estimate=pl.CostEstimate(flops=10000000000, bytes_accessed=8 << 20, transcendentals=0),
        name="edge",
    )(far(warmth), far(flag), far(floor))
    halos = tuple(
        lax.ppermute(edge, ("lat", "lon"), neighbours(lat, lon, first)) for first in range(2)
    )

    flow, warmth, flag, floor, basin = (near(x) for x in (flow, warmth, flag, floor, basin))
    half = pltpu.VMEM((dests // 2 * own_rows + shared_rows, LANES), jnp.float32)
    full = pltpu.VMEM((dests * own_rows + shared_rows, LANES), jnp.float32)
    results = ((half, half) if pairs else (full,)) + (
        pltpu.VMEM((levels, rows, cols), jnp.float32),
        pltpu.VMEM((rows, cols), jnp.float32),
    )
    room = pltpu.VMEM((7, levels, snapshots + 3, SUB, cols), jnp.float32)
    sums = pl.pallas_call(
        functools.partial(inner_kernel, dims, pairs),
        out_shape=results,
        in_specs=[vmem] * 5,
        out_specs=(vmem,) * len(results),
        scratch_shapes=[room],
        compiler_params=params,
        name="inner_rows",
    )(flow, warmth, flag, floor, basin)
    sums = pl.pallas_call(
        functools.partial(last_kernel, dims, pairs),
        out_shape=results,
        in_specs=[vmem] * (7 + len(results)),
        out_specs=(vmem,) * len(results),
        input_output_aliases={7 + i: i for i in range(len(results))},
        scratch_shapes=[room],
        compiler_params=params,
        name="last_rows",
    )(*halos[::-1], flow, warmth, flag, floor, basin, *sums)
    mean_warmth, limit = sums[-2:]

    if pairs:
        keep, give = sums[:2]
        came = lax.ppermute(give, "lon", [(i, i ^ 1) for i in range(lon)])
        message = pltpu.VMEM((own_rows + shared_rows, LANES), jnp.float32)
        chips = lon // 2
        messages = pl.pallas_call(
            functools.partial(pair_kernel, dims),
            out_shape=(message,) * chips,
            in_specs=[vmem, vmem],
            out_specs=(vmem,) * chips,
            compiler_params=params,
            name="pair_sums",
        )(keep, came)
        got = messages[:1] + tuple(
            lax.ppermute(messages[m], "lon", [(i, i ^ (2 * m + 1)) for i in range(lon)])
            for m in reversed(range(1, chips))
        )
    else:
        own, shared = sums[0][: dests * own_rows], sums[0][dests * own_rows :]
        sent = jnp.concatenate(
            [own.reshape(dests, own_rows, LANES), jnp.broadcast_to(shared, (dests, shared_rows, LANES))],
            axis=1,
        )
        if dests != lon:
            sent = jnp.repeat(sent, lon // dests, axis=0, total_repeat_length=lon)
        got = (lax.all_to_all(sent, "lon", 0, 0),)

    eddy, transport = pl.pallas_call(
        functools.partial(finish_kernel, dims, scaling),
        out_shape=(
            jax.ShapeDtypeStruct((levels, rows, cols), jnp.float32),
            jax.ShapeDtypeStruct((4, levels, per_dest * SUB, BASINS), jnp.float32),
        ),
        in_specs=[vmem] * (len(got) + 3),
        out_specs=(vmem, vmem),
        compiler_params=params,
        name="finish",
    )(*got, mean_warmth, limit, basin)
    if dests != lon:
        first = lax.axis_index("lon") * share % SUB
        transport = lax.dynamic_slice_in_dim(transport, first, share, 2)
    return eddy, jnp.transpose(transport, (0, 3, 1, 2))


def solution(mesh):
    return jax.shard_map(
        shards,
        mesh=mesh,
        in_specs=(
            P(None, None, "lat", "lon"),
            P(None, None, "lat", "lon"),
            P("lat", "lon"),
            P("lat", "lon"),
            P("lat", "lon"),
        ),
        out_specs=(P(None, "lat", "lon"), P(None, None, None, ("lat", "lon"))),
        check_vma=False,
    )
```

```python
import functools
import math

import jax
import jax.numpy as jnp
from jax import lax
from jax.experimental import pallas as pl
from jax.experimental.pallas import tpu as pltpu
from jax.sharding import PartitionSpec as P

BASINS = 10
SUB = 8
LANES = 128
CUT = 80
GRANT = 16 * 1024 * 1024


def cover(total, unit):
    return -(-total // unit)


def iota(axis):
    return lax.broadcasted_iota(jnp.int32, (SUB, LANES), axis)


def pick_lanes(tiles, start, width):
    first, shift = divmod(start, LANES)
    if shift == 0:
        return tiles[first]
    left = pltpu.roll(tiles[first], LANES - shift, 1)
    if shift + width <= LANES:
        return left
    right = pltpu.roll(tiles[first + 1], LANES - shift, 1)
    return jnp.where(lax.broadcasted_iota(jnp.int32, left.shape, 1) < LANES - shift, left, right)


def edge_kernel(dims, warmth, flag, floor, edge, rows_buf, flag_buf, floor_buf, sem):
    snapshots, levels = dims[:2]
    first = slice(0, SUB)
    copies = [
        pltpu.make_async_copy(flag.at[first, :], flag_buf, sem.at[snapshots]),
        pltpu.make_async_copy(floor.at[first, :], floor_buf, sem.at[snapshots + 1]),
    ] + [
        pltpu.make_async_copy(warmth.at[t, :, first, :], rows_buf.at[t], sem.at[t])
        for t in range(snapshots)
    ]
    for copy in copies:
        copy.start()
    for copy in copies:
        copy.wait()
    depth = (flag_buf[0:1, :] * floor_buf[0:1, :]).astype(jnp.float32)
    edge[snapshots * levels : snapshots * levels + 1, :] = depth
    for t in range(snapshots):
        for k in range(levels):
            edge[t * levels + k : t * levels + k + 1, :] = rows_buf[t, k, 0:1, :]


def prepare(dims, rows_of, room):
    snapshots, levels = dims[:2]
    get_v, get_w, put_mean = rows_of
    for k in range(levels):
        v = [get_v(t, k) for t in range(snapshots)]
        w = [get_w(t, k) for t in range(snapshots)]
        mv = sum(v[1:], v[0]) * (1.0 / snapshots)
        mw = sum(w[1:], w[0]) * (1.0 / snapshots)
        cross = sum((a - mv) * (b - mw) for a, b in zip(v, w)) * (1.0 / snapshots)
        put_mean(k, mw)
        for at, value in enumerate(w + [mv * mw, cross, mw]):
            room[k, at] = value


def multiply(dims, group, get_v, room, shallow, label):
    snapshots = dims[0]
    width = BASINS * SUB
    nothing = jnp.zeros((SUB, LANES), jnp.float32)

    def level_data(k):
        v = [get_v(t, k) for t in range(snapshots)]
        rest = [room[k, at] for at in range(snapshots + 3)]
        return jnp.concatenate(v + rest + [jnp.ones((SUB, LANES), jnp.float32)], axis=0)

    def level_hot(k):
        masked = jnp.where(shallow > float(k), label, -1)
        return [jnp.where(masked == b, 1.0, 0.0) for b in range(BASINS)]

    data = jnp.concatenate([level_data(k) for k in group], axis=1)
    columns = []
    for k in group:
        column = [nothing] * (group[0] * width % LANES // SUB)
        for other in group:
            column += level_hot(k) if other == k else [nothing] * BASINS
        columns.append(jnp.concatenate(column, axis=0))
    hot = jnp.concatenate(columns, axis=1).astype(jnp.bfloat16)
    exact, height = 2 * snapshots * SUB, data.shape[0]
    cuts = list(range(0, exact, CUT)) + [exact, height]
    parts, spans = [], []
    for at, end in zip(cuts, cuts[1:]):
        rest = data[at:end]
        count = 2 if at < exact else 3
        for piece in range(count):
            parts.append(rest.astype(jnp.bfloat16))
            if piece < count - 1:
                rest = rest - parts[-1].astype(jnp.float32)
        spans.append((end - at, count))
    dots = lax.dot_general(
        jnp.concatenate(parts, axis=0),
        hot,
        (((1,), (1,)), ((), ())),
        preferred_element_type=jnp.float32,
    )
    sums, at = [], 0
    for size, count in spans:
        x = dots[at : at + size]
        for piece in range(1, count):
            x = x + dots[at + piece * size : at + (piece + 1) * size]
        sums.append(x)
        at += size * count
    total = jnp.concatenate(sums, axis=0)
    spare = -total.shape[1] % LANES
    if spare:
        total = jnp.concatenate([total, jnp.zeros((total.shape[0], spare), jnp.float32)], axis=1)
    return total


def extract(dims, group, total, done):
    quantities = 2 * dims[0] + 4
    sub, lane = iota(0), iota(1)
    diagonal = lane % SUB
    tile, shift = divmod(group[0] * BASINS * SUB, LANES)
    for c in range(total.shape[1] // LANES):
        groups = []
        for g in range(quantities // SUB):
            acc = None
            for s in range(SUB):
                q = g * SUB + s
                row = jnp.take_along_axis(
                    total[q * SUB : (q + 1) * SUB, c * LANES : (c + 1) * LANES],
                    diagonal,
                    axis=0,
                    mode="promise_in_bounds",
                )
                acc = row if acc is None else jnp.where(sub == s, row, acc)
            if done[tile + c] is not None:
                acc = jnp.where(lane < shift, done[tile + c][g * SUB : (g + 1) * SUB], acc)
            groups.append(acc)
        done[tile + c] = jnp.concatenate(groups, axis=0)


def level_groups(dims):
    return [tuple(range(k, min(k + 2, dims[1]))) for k in range(0, dims[1], 2)]


def store_block(dims, n, done, keep, give):
    quantities = 2 * dims[0] + 4
    put_own, put_shared = writers(dims, n, keep, give)
    for c in range(dims[4]):
        put_own(c, done[c])
        for q in range(2):
            put_shared(c * 2 + q, done[c][quantities - 2 + q : quantities - 1 + q])


def writers(dims, n, keep, give):
    snapshots, levels, rows, blocks, tiles, dests, per_dest = dims
    quantities = 2 * snapshots + 4
    own_rows = tiles * quantities
    dest, inner = (n // per_dest, n % per_dest) if per_dest > 1 else (n, 0)
    halves = (keep,) if give is None else (keep, give)
    half = dest if give is None else dest // 2
    shared_at = keep.shape[0] - 2 * tiles * blocks

    def put_own(c, value):
        base = (half * per_dest + inner) * own_rows + c * quantities
        if not isinstance(base, int):
            base = pl.multiple_of(base, SUB)
        at = pl.ds(base, quantities)
        if give is None:
            keep[at, :] = value
            return
        me = lax.axis_index("lon")
        mine = (me % 2 == dest % 2) == (me // 2 == dest // 2)

        @pl.when(mine)
        def _():
            keep[at, :] = value

        @pl.when(jnp.logical_not(mine))
        def _():
            give[at, :] = value

    def put_shared(place, value):
        for ref in halves:
            ref[pl.ds(shared_at + place * blocks + n, 1), :] = value

    return put_own, put_shared


def inner_kernel(dims, pairs, flow, warmth, flag, floor, basin, *refs):
    blocks, tiles = dims[3:5]
    outs, room = refs[:-1], refs[-1]
    keep, give = outs[:2] if pairs else (outs[0], None)
    mean_warmth, limit = outs[-2:]

    def span(n):
        at = n * SUB if isinstance(n, int) else pl.multiple_of(n * SUB, SUB)
        return pl.ds(at, SUB), pl.ds(at + 1, SUB)

    def rows_of(n):
        here, north = span(n)

        def put_mean(k, value):
            mean_warmth[k, here, :] = value

        def get_v(t, k):
            return flow[t, k, here, :]

        def get_w(t, k):
            return 0.5 * (warmth[t, k, here, :] + warmth[t, k, north, :])

        return get_v, get_w, put_mean

    def several(ns):
        work = []
        for n in ns:
            here, north = span(n)
            depth = (flag[here, :] * floor[here, :]).astype(jnp.float32)
            upper = (flag[north, :] * floor[north, :]).astype(jnp.float32)
            shallow = jnp.minimum(depth, upper)
            limit[here, :] = shallow
            work.append((n, rows_of(n), shallow, basin[here, :], [None] * tiles))
        totals = []
        rooms = [room.at[i] for i in range(7)]
        for (n, rows, shallow, label, done), r in zip(work, rooms):
            prepare(dims, rows, r)
        for group in level_groups(dims):
            for (n, rows, shallow, label, done), r in zip(work, rooms):
                totals.append((group, done, multiply(dims, group, rows[0], r, shallow, label)))
        for group, done, total in totals:
            extract(dims, group, total, done)

        for n, _, _, _, done in work:
            store_block(dims, n, done, keep, give)

    def body(i, carry):
        several([i * 7 + j for j in range(7)])
        return carry

    lax.fori_loop(0, (blocks - 1) // 7, body, 0)
    rest = (blocks - 1) % 7
    if rest:
        several(list(range(blocks - 1 - rest, blocks - 1)))


def last_kernel(dims, pairs, odd_halo, even_halo, flow, warmth, flag, floor, basin, *refs):
    snapshots, levels, rows, blocks = dims[:4]
    refs, room = refs[:-1], refs[-1]
    outs = refs[len(refs) // 2 :]
    keep, give = outs[:2] if pairs else (outs[0], None)
    mean_warmth, limit = outs[-2:]
    here = slice(rows - SUB, rows)
    below = lax.broadcasted_iota(jnp.int32, (SUB, LANES), 0) < SUB - 1

    lat = lax.axis_index("lat")
    even = lat % 2 == 0
    inside = jnp.where(lat < lax.axis_size("lat") - 1, 1.0, 0.0)

    def north(block, n):
        row = jnp.where(even, even_halo[n : n + 1, :], odd_halo[n : n + 1, :]) * inside
        return jnp.where(below, pltpu.roll(block, SUB - 1, 0), row)

    depth = (flag[here, :] * floor[here, :]).astype(jnp.float32)
    edge_at = snapshots * levels
    shallow = jnp.minimum(depth, north(depth, edge_at))
    limit[here, :] = shallow

    def put_mean(k, value):
        mean_warmth[k, here, :] = value

    def get_v(t, k):
        return flow[t, k, here, :]

    def get_w(t, k):
        block = warmth[t, k, here, :]
        return 0.5 * (block + north(block, t * levels + k))

    room = room.at[0]
    prepare(dims, (get_v, get_w, put_mean), room)
    done = [None] * dims[4]
    for group in level_groups(dims):
        total = multiply(dims, group, get_v, room, shallow, basin[here, :])
        extract(dims, group, total, done)
    store_block(dims, blocks - 1, done, keep, give)


def spare_lanes(dims):
    snapshots, levels, rows, blocks, tiles, dests, per_dest = dims
    quantities = 2 * snapshots + 4
    used = levels * BASINS * SUB - (tiles - 1) * LANES
    fits = 2 * used <= LANES and 2 * blocks <= quantities - 4 and blocks % SUB == 0
    return fits, used, (tiles - 1) * quantities


def pair_kernel(dims, keep, came, *outs):
    tiles, per_dest = dims[4], dims[6]
    own_rows = per_dest * tiles * (2 * dims[0] + 4)
    chips = len(outs)
    shared = chips * own_rows
    chip = lax.axis_index("lon") // 2
    common = keep[shared:, :] + came[shared:, :]
    fits, used, start = spare_lanes(dims)
    for offset, out in enumerate(outs):
        at = pl.multiple_of((chip ^ offset) * own_rows, SUB)
        own = keep[pl.ds(at, own_rows), :] + came[pl.ds(at, own_rows), :]
        out[0:own_rows, :] = own
        if fits:
            rest = out.shape[0] - own_rows
            size = common.shape[0] - rest
            moved = pltpu.roll(common[rest:], used, 1)
            lane = lax.broadcasted_iota(jnp.int32, moved.shape, 1)
            out[start : start + size, :] = jnp.where(lane < used, own[start : start + size], moved)
            out[own_rows:, :] = common[:rest]
        else:
            out[own_rows:, :] = common


def finish_kernel(dims, scaling, packed, *refs):
    mean_warmth, limit, basin, eddy, transport = refs[-5:]
    snapshots, levels, rows, blocks, tiles, dests, per_dest = dims
    width = BASINS * SUB
    quantities = 2 * snapshots + 4
    own_rows = tiles * quantities
    sub, lane = iota(0), iota(1)
    got = refs[:-5]
    if len(got[0].shape) == 3:
        got = [got[0].at[d] for d in range(got[0].shape[0])]
    mine = got[0][...]
    for part in got[1:]:
        mine = mine + part[...]
    shared = mine[per_dest * own_rows :]
    if packed:
        _, used, start = spare_lanes(dims)
        beside = mine[start : start + 2 * blocks]
        shared = jnp.concatenate([shared, pltpu.roll(beside, LANES - used, 1)], axis=0)
    bar = []
    for c in range(tiles):
        at = c * 2 * blocks
        bar.append(shared[at : at + blocks] / jnp.maximum(shared[at + blocks : at + 2 * blocks], 1.0))
    for k in range(levels):
        level = pick_lanes(bar, k * width, width)
        for n in range(blocks):
            where = basin[n * SUB : (n + 1) * SUB, :] * SUB + sub
            row = jnp.broadcast_to(level[n : n + 1], (SUB, LANES))
            cell = jnp.take_along_axis(row, where, axis=1, mode="promise_in_bounds")
            deep = limit[n * SUB : (n + 1) * SUB, :] > float(k)
            star = mean_warmth[k, n * SUB : (n + 1) * SUB, :] - cell
            eddy[k, n * SUB : (n + 1) * SUB, :] = jnp.where(deep, star, 0.0)
    spread = jnp.minimum(lane, BASINS - 1) * SUB + sub
    for i in range(per_dest):
        terms = []
        for c in range(tiles):
            own = mine[i * own_rows + c * quantities : i * own_rows + (c + 1) * quantities]
            count = own[quantities - 1 : quantities]
            floor = jnp.maximum(count, 1.0)
            v = own[:snapshots] / floor
            w = own[snapshots : 2 * snapshots] / floor
            bar_v = jnp.sum(v, axis=0, keepdims=True) * (1.0 / snapshots)
            bar_w = jnp.sum(w, axis=0, keepdims=True) * (1.0 / snapshots)
            swing = jnp.sum((v - bar_v) * (w - bar_w), axis=0, keepdims=True) * (1.0 / snapshots)
            mean_part = count * bar_v * bar_w
            swing = count * swing
            product = own[2 * snapshots : 2 * snapshots + 1]
            cross = own[2 * snapshots + 1 : 2 * snapshots + 2]
            four = [mean_part, product - mean_part, swing, cross - swing]
            terms.append(scaling * jnp.concatenate(four + four, axis=0))
        for k in range(levels):
            level = pick_lanes(terms, k * width, width)
            for term in range(4):
                row = jnp.broadcast_to(level[term : term + 1], (SUB, LANES))
                cell = jnp.take_along_axis(row, spread, axis=1, mode="promise_in_bounds")
                transport[term, k, i * SUB : (i + 1) * SUB, :] = cell[:, :BASINS]


def neighbours(lat, lon, first):
    route = []
    for i in range(lat):
        other = i + 1 if (i - first) % 2 == 0 else i - 1
        for j in range(lon):
            across = j ^ 1 if lon % 2 == 0 else j
            if not 0 <= other < lat:
                target = i * lon + across
            elif other < i:
                target = other * lon + j
            else:
                target = other * lon + across
            route.append((i * lon + j, target))
    return route


def shards(flow, warmth, flag, floor, basin):
    snapshots, levels, rows, cols = flow.shape
    lon, lat = lax.axis_size("lon"), lax.axis_size("lat")
    scaling = 1.0 / math.sqrt(cols * lon)
    share = rows // lon
    blocks = rows // SUB
    per_dest = max(1, share // SUB)
    dests = blocks // per_dest
    width = BASINS * SUB
    tiles = cover(levels * width, LANES)
    quantities = 2 * snapshots + 4
    dims = (snapshots, levels, rows, blocks, tiles, dests, per_dest)
    own_rows, shared_rows = per_dest * tiles * quantities, tiles * 2 * blocks
    pairs = dests == lon and lon in (2, 4, 8)

    vmem = pl.BlockSpec(memory_space=pltpu.VMEM)
    hbm = pl.BlockSpec(memory_space=pl.ANY)
    params = pltpu.CompilerParams(vmem_limit_bytes=GRANT)

    def near(x):
        return pltpu.with_memory_space_constraint(x, pltpu.VMEM)

    def far(x):
        return pltpu.with_memory_space_constraint(x, pltpu.HBM)

    edge = pl.pallas_call(
        functools.partial(edge_kernel, dims),
        out_shape=pltpu.VMEM((snapshots * levels + 1, cols), jnp.float32),
        in_specs=[hbm] * 3,
        out_specs=vmem,
        scratch_shapes=[
            pltpu.VMEM((snapshots, levels, SUB, cols), jnp.float32),
            pltpu.VMEM((SUB, cols), jnp.int32),
            pltpu.VMEM((SUB, cols), jnp.int32),
            pltpu.SemaphoreType.DMA((snapshots + 2,)),
        ],
        compiler_params=params,
        cost_estimate=pl.CostEstimate(flops=10000000000, bytes_accessed=8 << 20, transcendentals=0),
        name="edge",
    )(far(warmth), far(flag), far(floor))
    halos = tuple(
        lax.ppermute(edge, ("lat", "lon"), neighbours(lat, lon, first)) for first in range(2)
    )

    flow, warmth, flag, floor, basin = (near(x) for x in (flow, warmth, flag, floor, basin))
    half = pltpu.VMEM((dests // 2 * own_rows + shared_rows, LANES), jnp.float32)
    full = pltpu.VMEM((dests * own_rows + shared_rows, LANES), jnp.float32)
    results = ((half, half) if pairs else (full,)) + (
        pltpu.VMEM((levels, rows, cols), jnp.float32),
        pltpu.VMEM((rows, cols), jnp.float32),
    )
    room = pltpu.VMEM((7, levels, snapshots + 3, SUB, cols), jnp.float32)
    sums = pl.pallas_call(
        functools.partial(inner_kernel, dims, pairs),
        out_shape=results,
        in_specs=[vmem] * 5,
        out_specs=(vmem,) * len(results),
        scratch_shapes=[room],
        compiler_params=params,
        name="inner_rows",
    )(flow, warmth, flag, floor, basin)
    sums = pl.pallas_call(
        functools.partial(last_kernel, dims, pairs),
        out_shape=results,
        in_specs=[vmem] * (7 + len(results)),
        out_specs=(vmem,) * len(results),
        input_output_aliases={7 + i: i for i in range(len(results))},
        scratch_shapes=[room],
        compiler_params=params,
        name="last_rows",
    )(*halos[::-1], flow, warmth, flag, floor, basin, *sums)
    mean_warmth, limit = sums[-2:]

    if pairs:
        keep, give = sums[:2]
        came = lax.ppermute(give, "lon", [(i, i ^ 1) for i in range(lon)])
        beside = 2 * blocks if spare_lanes(dims)[0] else 0
        message = pltpu.VMEM((own_rows + shared_rows - beside, LANES), jnp.float32)
        chips = lon // 2
        messages = pl.pallas_call(
            functools.partial(pair_kernel, dims),
            out_shape=(message,) * chips,
            in_specs=[vmem, vmem],
            out_specs=(vmem,) * chips,
            compiler_params=params,
            name="pair_sums",
        )(keep, came)
        got = messages[:1] + tuple(
            lax.ppermute(messages[m], "lon", [(i, i ^ (2 * m + 1)) for i in range(lon)])
            for m in reversed(range(1, chips))
        )
    else:
        own, shared = sums[0][: dests * own_rows], sums[0][dests * own_rows :]
        sent = jnp.concatenate(
            [own.reshape(dests, own_rows, LANES), jnp.broadcast_to(shared, (dests, shared_rows, LANES))],
            axis=1,
        )
        if dests != lon:
            sent = jnp.repeat(sent, lon // dests, axis=0, total_repeat_length=lon)
        got = (lax.all_to_all(sent, "lon", 0, 0),)

    eddy, transport = pl.pallas_call(
        functools.partial(finish_kernel, dims, scaling, pairs and spare_lanes(dims)[0]),
        out_shape=(
            jax.ShapeDtypeStruct((levels, rows, cols), jnp.float32),
            jax.ShapeDtypeStruct((4, levels, per_dest * SUB, BASINS), jnp.float32),
        ),
        in_specs=[vmem] * (len(got) + 3),
        out_specs=(vmem, vmem),
        compiler_params=params,
        name="finish",
    )(*got, mean_warmth, limit, basin)
    if dests != lon:
        first = lax.axis_index("lon") * share % SUB
        transport = lax.dynamic_slice_in_dim(transport, first, share, 2)
    return eddy, jnp.transpose(transport, (0, 3, 1, 2))


def solution(mesh):
    return jax.shard_map(
        shards,
        mesh=mesh,
        in_specs=(
            P(None, None, "lat", "lon"),
            P(None, None, "lat", "lon"),
            P("lat", "lon"),
            P("lat", "lon"),
            P("lat", "lon"),
        ),
        out_specs=(P(None, "lat", "lon"), P(None, None, None, ("lat", "lon"))),
        check_vma=False,
    )
```

```python
import functools
import math

import jax
import jax.numpy as jnp
from jax import lax
from jax.experimental import pallas as pl
from jax.experimental.pallas import tpu as pltpu
from jax.sharding import PartitionSpec as P

BASINS = 10
SUB = 8
LANES = 128
CUT = 32
GRANT = 16 * 1024 * 1024


def cover(total, unit):
    return -(-total // unit)


def iota(axis):
    return lax.broadcasted_iota(jnp.int32, (SUB, LANES), axis)


def pick_lanes(tiles, start, width):
    first, shift = divmod(start, LANES)
    if shift == 0:
        return tiles[first]
    left = pltpu.roll(tiles[first], LANES - shift, 1)
    if shift + width <= LANES:
        return left
    right = pltpu.roll(tiles[first + 1], LANES - shift, 1)
    return jnp.where(lax.broadcasted_iota(jnp.int32, left.shape, 1) < LANES - shift, left, right)


def edge_kernel(dims, warmth, flag, floor, edge, rows_buf, flag_buf, floor_buf, sem):
    snapshots, levels = dims[:2]
    first = slice(0, SUB)
    copies = [
        pltpu.make_async_copy(flag.at[first, :], flag_buf, sem.at[snapshots]),
        pltpu.make_async_copy(floor.at[first, :], floor_buf, sem.at[snapshots + 1]),
    ] + [
        pltpu.make_async_copy(warmth.at[t, :, first, :], rows_buf.at[t], sem.at[t])
        for t in range(snapshots)
    ]
    for copy in copies:
        copy.start()
    for copy in copies:
        copy.wait()
    depth = (flag_buf[0:1, :] * floor_buf[0:1, :]).astype(jnp.float32)
    edge[snapshots * levels : snapshots * levels + 1, :] = depth
    for t in range(snapshots):
        for k in range(levels):
            edge[t * levels + k : t * levels + k + 1, :] = rows_buf[t, k, 0:1, :]


def prepare(dims, rows_of, room):
    snapshots, levels = dims[:2]
    get_v, get_w, put_mean = rows_of
    for k in range(levels):
        v = [get_v(t, k) for t in range(snapshots)]
        w = [get_w(t, k) for t in range(snapshots)]
        mv = sum(v[1:], v[0]) * (1.0 / snapshots)
        mw = sum(w[1:], w[0]) * (1.0 / snapshots)
        cross = sum((a - mv) * (b - mw) for a, b in zip(v, w)) * (1.0 / snapshots)
        put_mean(k, mw)
        for at, value in enumerate(w + [mv * mw, cross, mw]):
            room[k, at] = value


def multiply(dims, group, get_v, room, shallow, label):
    snapshots = dims[0]
    width = BASINS * SUB
    nothing = jnp.zeros((SUB, LANES), jnp.float32)

    def level_data(k):
        v = [get_v(t, k) for t in range(snapshots)]
        rest = [room[k, at] for at in range(snapshots + 3)]
        return jnp.concatenate(v + rest + [jnp.ones((SUB, LANES), jnp.float32)], axis=0)

    def level_hot(k):
        masked = jnp.where(shallow > float(k), label, -1)
        return [jnp.where(masked == b, 1.0, 0.0) for b in range(BASINS)]

    data = jnp.concatenate([level_data(k) for k in group], axis=1)
    columns = []
    for k in group:
        column = [nothing] * (group[0] * width % LANES // SUB)
        for other in group:
            column += level_hot(k) if other == k else [nothing] * BASINS
        columns.append(jnp.concatenate(column, axis=0))
    hot = jnp.concatenate(columns, axis=1).astype(jnp.bfloat16)
    exact, height = 2 * snapshots * SUB, data.shape[0]
    cuts = list(range(0, exact, CUT)) + [exact, height]
    parts, spans = [], []
    for at, end in zip(cuts, cuts[1:]):
        rest = data[at:end]
        count = 2 if at < exact else 3
        for piece in range(count):
            parts.append(rest.astype(jnp.bfloat16))
            if piece < count - 1:
                rest = rest - parts[-1].astype(jnp.float32)
        spans.append((end - at, count))
    dots = lax.dot_general(
        jnp.concatenate(parts, axis=0),
        hot,
        (((1,), (1,)), ((), ())),
        preferred_element_type=jnp.float32,
    )
    sums, at = [], 0
    for size, count in spans:
        x = dots[at : at + size]
        for piece in range(1, count):
            x = x + dots[at + piece * size : at + (piece + 1) * size]
        sums.append(x)
        at += size * count
    total = jnp.concatenate(sums, axis=0)
    spare = -total.shape[1] % LANES
    if spare:
        total = jnp.concatenate([total, jnp.zeros((total.shape[0], spare), jnp.float32)], axis=1)
    return total


def extract(dims, group, total, done):
    quantities = 2 * dims[0] + 4
    sub, lane = iota(0), iota(1)
    diagonal = lane % SUB
    tile, shift = divmod(group[0] * BASINS * SUB, LANES)
    for c in range(total.shape[1] // LANES):
        groups = []
        for g in range(quantities // SUB):
            acc = None
            for s in range(SUB):
                q = g * SUB + s
                row = jnp.take_along_axis(
                    total[q * SUB : (q + 1) * SUB, c * LANES : (c + 1) * LANES],
                    diagonal,
                    axis=0,
                    mode="promise_in_bounds",
                )
                acc = row if acc is None else jnp.where(sub == s, row, acc)
            if done[tile + c] is not None:
                acc = jnp.where(lane < shift, done[tile + c][g * SUB : (g + 1) * SUB], acc)
            groups.append(acc)
        done[tile + c] = jnp.concatenate(groups, axis=0)


def level_groups(dims):
    return [tuple(range(k, min(k + 2, dims[1]))) for k in range(0, dims[1], 2)]


def store_block(dims, n, done, keep, give):
    quantities = 2 * dims[0] + 4
    put_own, put_shared = writers(dims, n, keep, give)
    for c in range(dims[4]):
        put_own(c, done[c])
        for q in range(2):
            put_shared(c * 2 + q, done[c][quantities - 2 + q : quantities - 1 + q])


def writers(dims, n, keep, give):
    snapshots, levels, rows, blocks, tiles, dests, per_dest = dims
    quantities = 2 * snapshots + 4
    own_rows = tiles * quantities
    dest, inner = (n // per_dest, n % per_dest) if per_dest > 1 else (n, 0)
    halves = (keep,) if give is None else (keep, give)
    half = dest if give is None else dest // 2
    shared_at = keep.shape[0] - 2 * tiles * blocks

    def put_own(c, value):
        base = (half * per_dest + inner) * own_rows + c * quantities
        if not isinstance(base, int):
            base = pl.multiple_of(base, SUB)
        at = pl.ds(base, quantities)
        if give is None:
            keep[at, :] = value
            return
        me = lax.axis_index("lon")
        mine = (me % 2 == dest % 2) == (me // 2 == dest // 2)

        @pl.when(mine)
        def _():
            keep[at, :] = value

        @pl.when(jnp.logical_not(mine))
        def _():
            give[at, :] = value

    def put_shared(place, value):
        for ref in halves:
            ref[pl.ds(shared_at + place * blocks + n, 1), :] = value

    return put_own, put_shared


def inner_kernel(dims, pairs, flow, warmth, flag, floor, basin, *refs):
    blocks, tiles = dims[3:5]
    outs, room = refs[:-1], refs[-1]
    keep, give = outs[:2] if pairs else (outs[0], None)
    mean_warmth, limit = outs[-2:]

    def span(n):
        at = n * SUB if isinstance(n, int) else pl.multiple_of(n * SUB, SUB)
        return pl.ds(at, SUB), pl.ds(at + 1, SUB)

    def rows_of(n):
        here, north = span(n)

        def put_mean(k, value):
            mean_warmth[k, here, :] = value

        def get_v(t, k):
            return flow[t, k, here, :]

        def get_w(t, k):
            return 0.5 * (warmth[t, k, here, :] + warmth[t, k, north, :])

        return get_v, get_w, put_mean

    def several(ns):
        work = []
        for n in ns:
            here, north = span(n)
            depth = (flag[here, :] * floor[here, :]).astype(jnp.float32)
            upper = (flag[north, :] * floor[north, :]).astype(jnp.float32)
            shallow = jnp.minimum(depth, upper)
            limit[here, :] = shallow
            work.append((n, rows_of(n), shallow, basin[here, :], [None] * tiles))
        totals = []
        rooms = [room.at[i] for i in range(7)]
        for (n, rows, shallow, label, done), r in zip(work, rooms):
            prepare(dims, rows, r)
        for group in level_groups(dims):
            for (n, rows, shallow, label, done), r in zip(work, rooms):
                totals.append((group, done, multiply(dims, group, rows[0], r, shallow, label)))
        for group, done, total in totals:
            extract(dims, group, total, done)

        for n, _, _, _, done in work:
            store_block(dims, n, done, keep, give)

    def body(i, carry):
        several([i * 7 + j for j in range(7)])
        return carry

    lax.fori_loop(0, (blocks - 1) // 7, body, 0)
    rest = (blocks - 1) % 7
    if rest:
        several(list(range(blocks - 1 - rest, blocks - 1)))


def last_kernel(dims, pairs, odd_halo, even_halo, flow, warmth, flag, floor, basin, *refs):
    snapshots, levels, rows, blocks = dims[:4]
    refs, room = refs[:-1], refs[-1]
    outs = refs[len(refs) // 2 :]
    keep, give = outs[:2] if pairs else (outs[0], None)
    mean_warmth, limit = outs[-2:]
    here = slice(rows - SUB, rows)
    below = lax.broadcasted_iota(jnp.int32, (SUB, LANES), 0) < SUB - 1

    lat = lax.axis_index("lat")
    even = lat % 2 == 0
    inside = jnp.where(lat < lax.axis_size("lat") - 1, 1.0, 0.0)

    def north(block, n):
        row = jnp.where(even, even_halo[n : n + 1, :], odd_halo[n : n + 1, :]) * inside
        return jnp.where(below, pltpu.roll(block, SUB - 1, 0), row)

    depth = (flag[here, :] * floor[here, :]).astype(jnp.float32)
    edge_at = snapshots * levels
    shallow = jnp.minimum(depth, north(depth, edge_at))
    limit[here, :] = shallow

    def put_mean(k, value):
        mean_warmth[k, here, :] = value

    def get_v(t, k):
        return flow[t, k, here, :]

    def get_w(t, k):
        block = warmth[t, k, here, :]
        return 0.5 * (block + north(block, t * levels + k))

    room = room.at[0]
    prepare(dims, (get_v, get_w, put_mean), room)
    done = [None] * dims[4]
    totals = [
        multiply(dims, group, get_v, room, shallow, basin[here, :]) for group in level_groups(dims)
    ]
    for group, total in zip(level_groups(dims), totals):
        extract(dims, group, total, done)
    store_block(dims, blocks - 1, done, keep, give)


def spare_lanes(dims):
    snapshots, levels, rows, blocks, tiles, dests, per_dest = dims
    quantities = 2 * snapshots + 4
    used = levels * BASINS * SUB - (tiles - 1) * LANES
    fits = 2 * used <= LANES and 2 * blocks <= quantities - 4 and blocks % SUB == 0
    return fits, used, (tiles - 1) * quantities


def pair_kernel(dims, keep, came, *outs):
    tiles, per_dest = dims[4], dims[6]
    own_rows = per_dest * tiles * (2 * dims[0] + 4)
    chips = len(outs)
    shared = chips * own_rows
    chip = lax.axis_index("lon") // 2
    common = keep[shared:, :] + came[shared:, :]
    fits, used, start = spare_lanes(dims)
    for offset, out in enumerate(outs):
        at = pl.multiple_of((chip ^ offset) * own_rows, SUB)
        own = keep[pl.ds(at, own_rows), :] + came[pl.ds(at, own_rows), :]
        out[0:own_rows, :] = own
        if fits:
            rest = out.shape[0] - own_rows
            size = common.shape[0] - rest
            moved = pltpu.roll(common[rest:], used, 1)
            lane = lax.broadcasted_iota(jnp.int32, moved.shape, 1)
            out[start : start + size, :] = jnp.where(lane < used, own[start : start + size], moved)
            out[own_rows:, :] = common[:rest]
        else:
            out[own_rows:, :] = common


def finish_kernel(dims, scaling, packed, *refs):
    mean_warmth, limit, basin, eddy_out, transport_out, eddy, transport, flat, sem = refs[-9:]
    snapshots, levels, rows, blocks, tiles, dests, per_dest = dims
    width = BASINS * SUB
    quantities = 2 * snapshots + 4
    own_rows = tiles * quantities
    sub, lane = iota(0), iota(1)
    got = refs[:-9]
    if len(got[0].shape) == 3:
        got = [got[0].at[d] for d in range(got[0].shape[0])]
    mine = got[0][...]
    for part in got[1:]:
        mine = mine + part[...]
    shared = mine[per_dest * own_rows :]
    if packed:
        _, used, start = spare_lanes(dims)
        beside = mine[start : start + 2 * blocks]
        shared = jnp.concatenate([shared, pltpu.roll(beside, LANES - used, 1)], axis=0)
    bar = []
    for c in range(tiles):
        at = c * 2 * blocks
        bar.append(shared[at : at + blocks] / jnp.maximum(shared[at + blocks : at + 2 * blocks], 1.0))
    for k in range(levels):
        flat[k] = pick_lanes(bar, k * width, width)
    copies = []
    for k in range(levels):
        for n in range(blocks):
            where = basin[n * SUB : (n + 1) * SUB, :] * SUB + sub
            row = jnp.broadcast_to(flat[k, n : n + 1, :], (SUB, LANES))
            cell = jnp.take_along_axis(row, where, axis=1, mode="promise_in_bounds")
            deep = limit[n * SUB : (n + 1) * SUB, :] > float(k)
            star = mean_warmth[k, n * SUB : (n + 1) * SUB, :] - cell
            eddy[k, n * SUB : (n + 1) * SUB, :] = jnp.where(deep, star, 0.0)
        copies.append(pltpu.make_async_copy(eddy.at[k], eddy_out.at[k], sem.at[k]))
        copies[-1].start()
    spread = jnp.minimum(lane, BASINS - 1) * SUB + sub
    for i in range(per_dest):
        terms = []
        for c in range(tiles):
            own = mine[i * own_rows + c * quantities : i * own_rows + (c + 1) * quantities]
            count = own[quantities - 1 : quantities]
            floor = jnp.maximum(count, 1.0)
            v = own[:snapshots] / floor
            w = own[snapshots : 2 * snapshots] / floor
            bar_v = jnp.sum(v, axis=0, keepdims=True) * (1.0 / snapshots)
            bar_w = jnp.sum(w, axis=0, keepdims=True) * (1.0 / snapshots)
            swing = jnp.sum((v - bar_v) * (w - bar_w), axis=0, keepdims=True) * (1.0 / snapshots)
            mean_part = count * bar_v * bar_w
            swing = count * swing
            product = own[2 * snapshots : 2 * snapshots + 1]
            cross = own[2 * snapshots + 1 : 2 * snapshots + 2]
            four = [mean_part, product - mean_part, swing, cross - swing]
            terms.append(scaling * jnp.concatenate(four + four, axis=0))
        for k in range(levels):
            level = pick_lanes(terms, k * width, width)
            for term in range(4):
                row = jnp.broadcast_to(level[term : term + 1], (SUB, LANES))
                cell = jnp.take_along_axis(row, spread, axis=1, mode="promise_in_bounds")
                transport[term, k, i * SUB : (i + 1) * SUB, :] = cell[:, :BASINS]
    copies.append(pltpu.make_async_copy(transport, transport_out, sem.at[levels]))
    copies[-1].start()
    for copy in copies:
        copy.wait()


def neighbours(lat, lon, first):
    route = []
    for i in range(lat):
        other = i + 1 if (i - first) % 2 == 0 else i - 1
        for j in range(lon):
            across = j ^ 1 if lon % 2 == 0 else j
            if not 0 <= other < lat:
                target = i * lon + across
            elif other < i:
                target = other * lon + j
            else:
                target = other * lon + across
            route.append((i * lon + j, target))
    return route


def shards(flow, warmth, flag, floor, basin):
    snapshots, levels, rows, cols = flow.shape
    lon, lat = lax.axis_size("lon"), lax.axis_size("lat")
    scaling = 1.0 / math.sqrt(cols * lon)
    share = rows // lon
    blocks = rows // SUB
    per_dest = max(1, share // SUB)
    dests = blocks // per_dest
    width = BASINS * SUB
    tiles = cover(levels * width, LANES)
    quantities = 2 * snapshots + 4
    dims = (snapshots, levels, rows, blocks, tiles, dests, per_dest)
    own_rows, shared_rows = per_dest * tiles * quantities, tiles * 2 * blocks
    pairs = dests == lon and lon in (2, 4, 8)

    vmem = pl.BlockSpec(memory_space=pltpu.VMEM)
    hbm = pl.BlockSpec(memory_space=pl.ANY)
    params = pltpu.CompilerParams(vmem_limit_bytes=GRANT)

    def near(x):
        return pltpu.with_memory_space_constraint(x, pltpu.VMEM)

    def far(x):
        return pltpu.with_memory_space_constraint(x, pltpu.HBM)

    edge = pl.pallas_call(
        functools.partial(edge_kernel, dims),
        out_shape=pltpu.VMEM((snapshots * levels + 1, cols), jnp.float32),
        in_specs=[hbm] * 3,
        out_specs=vmem,
        scratch_shapes=[
            pltpu.VMEM((snapshots, levels, SUB, cols), jnp.float32),
            pltpu.VMEM((SUB, cols), jnp.int32),
            pltpu.VMEM((SUB, cols), jnp.int32),
            pltpu.SemaphoreType.DMA((snapshots + 2,)),
        ],
        compiler_params=params,
        cost_estimate=pl.CostEstimate(flops=10000000000, bytes_accessed=8 << 20, transcendentals=0),
        name="edge",
    )(far(warmth), far(flag), far(floor))
    halos = tuple(
        lax.ppermute(edge, ("lat", "lon"), neighbours(lat, lon, first)) for first in range(2)
    )

    flow, warmth, flag, floor, basin = (near(x) for x in (flow, warmth, flag, floor, basin))
    half = pltpu.VMEM((dests // 2 * own_rows + shared_rows, LANES), jnp.float32)
    full = pltpu.VMEM((dests * own_rows + shared_rows, LANES), jnp.float32)
    results = ((half, half) if pairs else (full,)) + (
        pltpu.VMEM((levels, rows, cols), jnp.float32),
        pltpu.VMEM((rows, cols), jnp.float32),
    )
    room = pltpu.VMEM((7, levels, snapshots + 3, SUB, cols), jnp.float32)
    sums = pl.pallas_call(
        functools.partial(inner_kernel, dims, pairs),
        out_shape=results,
        in_specs=[vmem] * 5,
        out_specs=(vmem,) * len(results),
        scratch_shapes=[room],
        compiler_params=params,
        name="inner_rows",
    )(flow, warmth, flag, floor, basin)
    sums = pl.pallas_call(
        functools.partial(last_kernel, dims, pairs),
        out_shape=results,
        in_specs=[vmem] * (7 + len(results)),
        out_specs=(vmem,) * len(results),
        input_output_aliases={7 + i: i for i in range(len(results))},
        scratch_shapes=[room],
        compiler_params=params,
        name="last_rows",
    )(*halos[::-1], flow, warmth, flag, floor, basin, *sums)
    mean_warmth, limit = sums[-2:]

    if pairs:
        keep, give = sums[:2]
        came = lax.ppermute(give, "lon", [(i, i ^ 1) for i in range(lon)])
        beside = 2 * blocks if spare_lanes(dims)[0] else 0
        message = pltpu.VMEM((own_rows + shared_rows - beside, LANES), jnp.float32)
        chips = lon // 2
        messages = pl.pallas_call(
            functools.partial(pair_kernel, dims),
            out_shape=(message,) * chips,
            in_specs=[vmem, vmem],
            out_specs=(vmem,) * chips,
            compiler_params=params,
            name="pair_sums",
        )(keep, came)
        got = messages[:1] + tuple(
            lax.ppermute(messages[m], "lon", [(i, i ^ (2 * m + 1)) for i in range(lon)])
            for m in reversed(range(1, chips))
        )
    else:
        own, shared = sums[0][: dests * own_rows], sums[0][dests * own_rows :]
        sent = jnp.concatenate(
            [own.reshape(dests, own_rows, LANES), jnp.broadcast_to(shared, (dests, shared_rows, LANES))],
            axis=1,
        )
        if dests != lon:
            sent = jnp.repeat(sent, lon // dests, axis=0, total_repeat_length=lon)
        got = (lax.all_to_all(sent, "lon", 0, 0),)

    outputs = ((levels, rows, cols), (4, levels, per_dest * SUB, BASINS))
    eddy, transport = pl.pallas_call(
        functools.partial(finish_kernel, dims, scaling, pairs and spare_lanes(dims)[0]),
        out_shape=tuple(pltpu.HBM(shape, jnp.float32) for shape in outputs),
        in_specs=[vmem] * (len(got) + 3),
        out_specs=(hbm, hbm),
        scratch_shapes=[pltpu.VMEM(shape, jnp.float32) for shape in outputs]
        + [
            pltpu.VMEM((levels, blocks, LANES), jnp.float32),
            pltpu.SemaphoreType.DMA((levels + 1,)),
        ],
        compiler_params=params,
        name="finish",
    )(*got, mean_warmth, limit, basin)
    if dests != lon:
        first = lax.axis_index("lon") * share % SUB
        transport = lax.dynamic_slice_in_dim(transport, first, share, 2)
    return eddy, jnp.transpose(transport, (0, 3, 1, 2))


def solution(mesh):
    return jax.shard_map(
        shards,
        mesh=mesh,
        in_specs=(
            P(None, None, "lat", "lon"),
            P(None, None, "lat", "lon"),
            P("lat", "lon"),
            P("lat", "lon"),
            P("lat", "lon"),
        ),
        out_specs=(P(None, "lat", "lon"), P(None, None, None, ("lat", "lon"))),
        check_vma=False,
    )
```

```python
import functools
import math

import jax
import jax.numpy as jnp
from jax import lax
from jax.experimental import pallas as pl
from jax.experimental.pallas import tpu as pltpu
from jax.sharding import PartitionSpec as P

BASINS = 10
SUB = 8
LANES = 128
CUT = 32
GRANT = 16 * 1024 * 1024


def cover(total, unit):
    return -(-total // unit)


def iota(axis):
    return lax.broadcasted_iota(jnp.int32, (SUB, LANES), axis)


def pick_lanes(tiles, start, width):
    first, shift = divmod(start, LANES)
    if shift == 0:
        return tiles[first]
    left = pltpu.roll(tiles[first], LANES - shift, 1)
    if shift + width <= LANES:
        return left
    right = pltpu.roll(tiles[first + 1], LANES - shift, 1)
    return jnp.where(lax.broadcasted_iota(jnp.int32, left.shape, 1) < LANES - shift, left, right)


def edge_kernel(dims, warmth, flag, floor, edge, rows_buf, flag_buf, floor_buf, sem):
    snapshots, levels = dims[:2]
    first = slice(0, SUB)
    copies = [
        pltpu.make_async_copy(flag.at[first, :], flag_buf, sem.at[snapshots]),
        pltpu.make_async_copy(floor.at[first, :], floor_buf, sem.at[snapshots + 1]),
    ] + [
        pltpu.make_async_copy(warmth.at[t, :, first, :], rows_buf.at[t], sem.at[t])
        for t in range(snapshots)
    ]
    for copy in copies:
        copy.start()
    for copy in copies:
        copy.wait()
    depth = (flag_buf[0:1, :] * floor_buf[0:1, :]).astype(jnp.float32)
    edge[snapshots * levels : snapshots * levels + 1, :] = depth
    for t in range(snapshots):
        for k in range(levels):
            edge[t * levels + k : t * levels + k + 1, :] = rows_buf[t, k, 0:1, :]


def prepare(dims, rows_of, room):
    snapshots, levels = dims[:2]
    get_v, get_w, put_mean = rows_of
    for k in range(levels):
        v = [get_v(t, k) for t in range(snapshots)]
        w = [get_w(t, k) for t in range(snapshots)]
        mv = sum(v[1:], v[0]) * (1.0 / snapshots)
        mw = sum(w[1:], w[0]) * (1.0 / snapshots)
        cross = sum((a - mv) * (b - mw) for a, b in zip(v, w)) * (1.0 / snapshots)
        put_mean(k, mw)
        for at, value in enumerate(w + [mv * mw, cross, mw]):
            room[k, at] = value


def multiply(dims, group, get_v, room, shallow, label):
    snapshots = dims[0]
    width = BASINS * SUB
    nothing = jnp.zeros((SUB, LANES), jnp.float32)

    def level_data(k):
        v = [get_v(t, k) for t in range(snapshots)]
        rest = [room[k, at] for at in range(snapshots + 3)]
        return jnp.concatenate(v + rest + [jnp.ones((SUB, LANES), jnp.float32)], axis=0)

    def level_hot(k):
        masked = jnp.where(shallow > float(k), label, -1)
        return [jnp.where(masked == b, 1.0, 0.0) for b in range(BASINS)]

    data = jnp.concatenate([level_data(k) for k in group], axis=1)
    columns = []
    for k in group:
        column = [nothing] * (group[0] * width % LANES // SUB)
        for other in group:
            column += level_hot(k) if other == k else [nothing] * BASINS
        columns.append(jnp.concatenate(column, axis=0))
    hot = jnp.concatenate(columns, axis=1).astype(jnp.bfloat16)
    exact, height = 2 * snapshots * SUB, data.shape[0]
    cuts = list(range(0, exact, CUT)) + [exact, height]
    parts, spans = [], []
    for at, end in zip(cuts, cuts[1:]):
        rest = data[at:end]
        count = 2 if at < exact else 3
        for piece in range(count):
            parts.append(rest.astype(jnp.bfloat16))
            if piece < count - 1:
                rest = rest - parts[-1].astype(jnp.float32)
        spans.append((end - at, count))
    dots = lax.dot_general(
        jnp.concatenate(parts, axis=0),
        hot,
        (((1,), (1,)), ((), ())),
        preferred_element_type=jnp.float32,
    )
    sums, at = [], 0
    for size, count in spans:
        x = dots[at : at + size]
        for piece in range(1, count):
            x = x + dots[at + piece * size : at + (piece + 1) * size]
        sums.append(x)
        at += size * count
    total = jnp.concatenate(sums, axis=0)
    spare = -total.shape[1] % LANES
    if spare:
        total = jnp.concatenate([total, jnp.zeros((total.shape[0], spare), jnp.float32)], axis=1)
    return total


def extract(dims, group, total, done):
    quantities = 2 * dims[0] + 4
    sub, lane = iota(0), iota(1)
    diagonal = lane % SUB
    tile, shift = divmod(group[0] * BASINS * SUB, LANES)
    for c in range(total.shape[1] // LANES):
        groups = []
        for g in range(quantities // SUB):
            acc = None
            for s in range(SUB):
                q = g * SUB + s
                row = jnp.take_along_axis(
                    total[q * SUB : (q + 1) * SUB, c * LANES : (c + 1) * LANES],
                    diagonal,
                    axis=0,
                    mode="promise_in_bounds",
                )
                acc = row if acc is None else jnp.where(sub == s, row, acc)
            if done[tile + c] is not None:
                acc = jnp.where(lane < shift, done[tile + c][g * SUB : (g + 1) * SUB], acc)
            groups.append(acc)
        done[tile + c] = jnp.concatenate(groups, axis=0)


def level_groups(dims):
    return [tuple(range(k, min(k + 2, dims[1]))) for k in range(0, dims[1], 2)]


def store_block(dims, n, done, keep, give):
    quantities = 2 * dims[0] + 4
    put_own, put_shared = writers(dims, n, keep, give)
    for c in range(dims[4]):
        put_own(c, done[c])
        for q in range(2):
            put_shared(c * 2 + q, done[c][quantities - 2 + q : quantities - 1 + q])


def writers(dims, n, keep, give):
    snapshots, levels, rows, blocks, tiles, dests, per_dest = dims
    quantities = 2 * snapshots + 4
    own_rows = tiles * quantities
    dest, inner = (n // per_dest, n % per_dest) if per_dest > 1 else (n, 0)
    halves = (keep,) if give is None else (keep, give)
    half = dest if give is None else dest // 2
    shared_at = keep.shape[0] - 2 * tiles * blocks

    def put_own(c, value):
        base = (half * per_dest + inner) * own_rows + c * quantities
        if not isinstance(base, int):
            base = pl.multiple_of(base, SUB)
        at = pl.ds(base, quantities)
        if give is None:
            keep[at, :] = value
            return
        me = lax.axis_index("lon")
        mine = (me % 2 == dest % 2) == (me // 2 == dest // 2)

        @pl.when(mine)
        def _():
            keep[at, :] = value

        @pl.when(jnp.logical_not(mine))
        def _():
            give[at, :] = value

    def put_shared(place, value):
        for ref in halves:
            ref[pl.ds(shared_at + place * blocks + n, 1), :] = value

    return put_own, put_shared


def inner_kernel(dims, pairs, flow, warmth, flag, floor, basin, *refs):
    blocks, tiles = dims[3:5]
    outs, room = refs[:-1], refs[-1]
    keep, give = outs[:2] if pairs else (outs[0], None)
    mean_warmth, limit = outs[-2:]

    def span(n):
        at = n * SUB if isinstance(n, int) else pl.multiple_of(n * SUB, SUB)
        return pl.ds(at, SUB), pl.ds(at + 1, SUB)

    def rows_of(n):
        here, north = span(n)

        def put_mean(k, value):
            mean_warmth[k, here, :] = value

        def get_v(t, k):
            return flow[t, k, here, :]

        def get_w(t, k):
            return 0.5 * (warmth[t, k, here, :] + warmth[t, k, north, :])

        return get_v, get_w, put_mean

    def several(ns):
        work = []
        for n in ns:
            here, north = span(n)
            depth = (flag[here, :] * floor[here, :]).astype(jnp.float32)
            upper = (flag[north, :] * floor[north, :]).astype(jnp.float32)
            shallow = jnp.minimum(depth, upper)
            limit[here, :] = shallow
            work.append((n, rows_of(n), shallow, basin[here, :], [None] * tiles))
        totals = []
        rooms = [room.at[i] for i in range(7)]
        for (n, rows, shallow, label, done), r in zip(work, rooms):
            prepare(dims, rows, r)
        for group in level_groups(dims):
            for (n, rows, shallow, label, done), r in zip(work, rooms):
                totals.append((group, done, multiply(dims, group, rows[0], r, shallow, label)))
        for group, done, total in totals:
            extract(dims, group, total, done)

        for n, _, _, _, done in work:
            store_block(dims, n, done, keep, give)

    def body(i, carry):
        several([i * 7 + j for j in range(7)])
        return carry

    lax.fori_loop(0, (blocks - 1) // 7, body, 0)
    rest = (blocks - 1) % 7
    if rest:
        several(list(range(blocks - 1 - rest, blocks - 1)))


def last_kernel(dims, pairs, odd_halo, even_halo, flow, warmth, flag, floor, basin, *refs):
    snapshots, levels, rows, blocks = dims[:4]
    refs, room = refs[:-1], refs[-1]
    outs = refs[len(refs) // 2 :]
    keep, give = outs[:2] if pairs else (outs[0], None)
    mean_warmth, limit = outs[-2:]
    here = slice(rows - SUB, rows)
    below = lax.broadcasted_iota(jnp.int32, (SUB, LANES), 0) < SUB - 1

    lat = lax.axis_index("lat")
    even = lat % 2 == 0
    inside = jnp.where(lat < lax.axis_size("lat") - 1, 1.0, 0.0)

    def north(block, n):
        row = jnp.where(even, even_halo[n : n + 1, :], odd_halo[n : n + 1, :]) * inside
        return jnp.where(below, pltpu.roll(block, SUB - 1, 0), row)

    depth = (flag[here, :] * floor[here, :]).astype(jnp.float32)
    edge_at = snapshots * levels
    shallow = jnp.minimum(depth, north(depth, edge_at))
    limit[here, :] = shallow

    def put_mean(k, value):
        mean_warmth[k, here, :] = value

    def get_v(t, k):
        return flow[t, k, here, :]

    def get_w(t, k):
        block = warmth[t, k, here, :]
        return 0.5 * (block + north(block, t * levels + k))

    room = room.at[0]
    prepare(dims, (get_v, get_w, put_mean), room)
    done = [None] * dims[4]
    totals = [
        multiply(dims, group, get_v, room, shallow, basin[here, :]) for group in level_groups(dims)
    ]
    for group, total in zip(level_groups(dims), totals):
        extract(dims, group, total, done)
    store_block(dims, blocks - 1, done, keep, give)


def spare_lanes(dims):
    snapshots, levels, rows, blocks, tiles, dests, per_dest = dims
    quantities = 2 * snapshots + 4
    used = levels * BASINS * SUB - (tiles - 1) * LANES
    fits = 2 * used <= LANES and 2 * blocks <= quantities - 4 and blocks % SUB == 0
    return fits, used, (tiles - 1) * quantities


def pair_kernel(dims, keep, came, *outs):
    tiles, per_dest = dims[4], dims[6]
    own_rows = per_dest * tiles * (2 * dims[0] + 4)
    chips = len(outs)
    shared = chips * own_rows
    chip = lax.axis_index("lon") // 2
    common = keep[shared:, :] + came[shared:, :]
    fits, used, start = spare_lanes(dims)
    for offset, out in enumerate(outs):
        at = pl.multiple_of((chip ^ offset) * own_rows, SUB)
        own = keep[pl.ds(at, own_rows), :] + came[pl.ds(at, own_rows), :]
        out[0:own_rows, :] = own
        if fits:
            rest = out.shape[0] - own_rows
            size = common.shape[0] - rest
            moved = pltpu.roll(common[rest:], used, 1)
            lane = lax.broadcasted_iota(jnp.int32, moved.shape, 1)
            out[start : start + size, :] = jnp.where(lane < used, own[start : start + size], moved)
            out[own_rows:, :] = common[:rest]
        else:
            out[own_rows:, :] = common


def finish_kernel(dims, scaling, packed, *refs):
    mean_warmth, limit, basin, eddy_out, transport_out, eddy, transport, flat, sem = refs[-9:]
    snapshots, levels, rows, blocks, tiles, dests, per_dest = dims
    width = BASINS * SUB
    quantities = 2 * snapshots + 4
    own_rows = tiles * quantities
    sub, lane = iota(0), iota(1)
    got = refs[:-9]
    if len(got[0].shape) == 3:
        got = [got[0].at[d] for d in range(got[0].shape[0])]
    mine = got[0][...]
    for part in got[1:]:
        mine = mine + part[...]
    shared = mine[per_dest * own_rows :]
    if packed:
        _, used, start = spare_lanes(dims)
        beside = mine[start : start + 2 * blocks]
        shared = jnp.concatenate([shared, pltpu.roll(beside, LANES - used, 1)], axis=0)
    bar = []
    for c in range(tiles):
        at = c * 2 * blocks
        bar.append(shared[at : at + blocks] / jnp.maximum(shared[at + blocks : at + 2 * blocks], 1.0))
    for k in range(levels):
        flat[k] = pick_lanes(bar, k * width, width)
    copies = []
    for k in range(levels):
        for n in range(blocks):
            where = basin[n * SUB : (n + 1) * SUB, :] * SUB + sub
            row = jnp.broadcast_to(flat[k, n : n + 1, :], (SUB, LANES))
            cell = jnp.take_along_axis(row, where, axis=1, mode="promise_in_bounds")
            deep = limit[n * SUB : (n + 1) * SUB, :] > float(k)
            star = mean_warmth[k, n * SUB : (n + 1) * SUB, :] - cell
            eddy[k, n * SUB : (n + 1) * SUB, :] = jnp.where(deep, star, 0.0)
        copies.append(pltpu.make_async_copy(eddy.at[k], eddy_out.at[k], sem.at[k]))
        copies[-1].start()
    spread = jnp.minimum(lane, BASINS - 1) * SUB + sub
    for i in range(per_dest):
        terms = []
        for c in range(tiles):
            own = mine[i * own_rows + c * quantities : i * own_rows + (c + 1) * quantities]
            count = own[quantities - 1 : quantities]
            floor = jnp.maximum(count, 1.0)
            v = own[:snapshots] / floor
            w = own[snapshots : 2 * snapshots] / floor
            bar_v = jnp.sum(v, axis=0, keepdims=True) * (1.0 / snapshots)
            bar_w = jnp.sum(w, axis=0, keepdims=True) * (1.0 / snapshots)
            swing = jnp.sum((v - bar_v) * (w - bar_w), axis=0, keepdims=True) * (1.0 / snapshots)
            mean_part = count * bar_v * bar_w
            swing = count * swing
            product = own[2 * snapshots : 2 * snapshots + 1]
            cross = own[2 * snapshots + 1 : 2 * snapshots + 2]
            four = [mean_part, product - mean_part, swing, cross - swing]
            terms.append(scaling * jnp.concatenate(four + four, axis=0))
        for k in range(levels):
            level = pick_lanes(terms, k * width, width)
            for term in range(4):
                row = jnp.broadcast_to(level[term : term + 1], (SUB, LANES))
                cell = jnp.take_along_axis(row, spread, axis=1, mode="promise_in_bounds")
                transport[term, k, i * SUB : (i + 1) * SUB, :] = cell[:, :BASINS]
    copies.append(pltpu.make_async_copy(transport, transport_out, sem.at[levels]))
    copies[-1].start()
    for copy in copies:
        copy.wait()


def neighbours(lat, lon, first):
    route = []
    for i in range(lat):
        other = i + 1 if (i - first) % 2 == 0 else i - 1
        for j in range(lon):
            across = j ^ 1 if lon % 2 == 0 else j
            if not 0 <= other < lat:
                target = i * lon + across
            elif other < i:
                target = other * lon + j
            else:
                target = other * lon + across
            route.append((i * lon + j, target))
    return route


def shards(flow, warmth, flag, floor, basin):
    snapshots, levels, rows, cols = flow.shape
    lon, lat = lax.axis_size("lon"), lax.axis_size("lat")
    scaling = 1.0 / math.sqrt(cols * lon)
    share = rows // lon
    blocks = rows // SUB
    per_dest = max(1, share // SUB)
    dests = blocks // per_dest
    width = BASINS * SUB
    tiles = cover(levels * width, LANES)
    quantities = 2 * snapshots + 4
    dims = (snapshots, levels, rows, blocks, tiles, dests, per_dest)
    own_rows, shared_rows = per_dest * tiles * quantities, tiles * 2 * blocks
    pairs = dests == lon and lon in (2, 4, 8)

    vmem = pl.BlockSpec(memory_space=pltpu.VMEM)
    hbm = pl.BlockSpec(memory_space=pl.ANY)
    params = pltpu.CompilerParams(vmem_limit_bytes=GRANT)

    def near(x):
        return pltpu.with_memory_space_constraint(x, pltpu.VMEM)

    def far(x):
        return pltpu.with_memory_space_constraint(x, pltpu.HBM)

    edge = pl.pallas_call(
        functools.partial(edge_kernel, dims),
        out_shape=pltpu.VMEM((snapshots * levels + 1, cols), jnp.float32),
        in_specs=[hbm] * 3,
        out_specs=vmem,
        scratch_shapes=[
            pltpu.VMEM((snapshots, levels, SUB, cols), jnp.float32),
            pltpu.VMEM((SUB, cols), jnp.int32),
            pltpu.VMEM((SUB, cols), jnp.int32),
            pltpu.SemaphoreType.DMA((snapshots + 2,)),
        ],
        compiler_params=params,
        cost_estimate=pl.CostEstimate(flops=10000000000, bytes_accessed=8 << 20, transcendentals=0),
        name="edge",
    )(far(warmth), far(flag), far(floor))
    halos = tuple(
        lax.ppermute(edge, ("lat", "lon"), neighbours(lat, lon, first)) for first in range(2)
    )

    flow, warmth, flag, floor, basin = (near(x) for x in (flow, warmth, flag, floor, basin))
    half = pltpu.VMEM((dests // 2 * own_rows + shared_rows, LANES), jnp.float32)
    full = pltpu.VMEM((dests * own_rows + shared_rows, LANES), jnp.float32)
    results = ((half, half) if pairs else (full,)) + (
        pltpu.VMEM((levels, rows, cols), jnp.float32),
        pltpu.VMEM((rows, cols), jnp.float32),
    )
    room = pltpu.VMEM((7, levels, snapshots + 3, SUB, cols), jnp.float32)
    sums = pl.pallas_call(
        functools.partial(inner_kernel, dims, pairs),
        out_shape=results,
        in_specs=[vmem] * 5,
        out_specs=(vmem,) * len(results),
        scratch_shapes=[room],
        compiler_params=params,
        name="inner_rows",
    )(flow, warmth, flag, floor, basin)
    sums = pl.pallas_call(
        functools.partial(last_kernel, dims, pairs),
        out_shape=results,
        in_specs=[vmem] * (7 + len(results)),
        out_specs=(vmem,) * len(results),
        input_output_aliases={7 + i: i for i in range(len(results))},
        scratch_shapes=[room],
        compiler_params=params,
        name="last_rows",
    )(*halos[::-1], flow, warmth, flag, floor, basin, *sums)
    mean_warmth, limit = sums[-2:]

    if pairs:
        keep, give = sums[:2]
        came = lax.ppermute(give, "lon", [(i, i ^ 1) for i in range(lon)])
        beside = 2 * blocks if spare_lanes(dims)[0] else 0
        message = pltpu.VMEM((own_rows + shared_rows - beside, LANES), jnp.float32)
        chips = lon // 2
        messages = pl.pallas_call(
            functools.partial(pair_kernel, dims),
            out_shape=(message,) * chips,
            in_specs=[vmem, vmem],
            out_specs=(vmem,) * chips,
            compiler_params=params,
            name="pair_sums",
        )(keep, came)
        far_first = list(reversed(range(1, chips)))
        order = far_first[1:2] + far_first[:1] + far_first[2:]
        got = messages[:1] + tuple(
            lax.ppermute(messages[m], "lon", [(i, i ^ (2 * m + 1)) for i in range(lon)])
            for m in order
        )
    else:
        own, shared = sums[0][: dests * own_rows], sums[0][dests * own_rows :]
        sent = jnp.concatenate(
            [own.reshape(dests, own_rows, LANES), jnp.broadcast_to(shared, (dests, shared_rows, LANES))],
            axis=1,
        )
        if dests != lon:
            sent = jnp.repeat(sent, lon // dests, axis=0, total_repeat_length=lon)
        got = (lax.all_to_all(sent, "lon", 0, 0),)

    outputs = ((levels, rows, cols), (4, levels, per_dest * SUB, BASINS))
    eddy, transport = pl.pallas_call(
        functools.partial(finish_kernel, dims, scaling, pairs and spare_lanes(dims)[0]),
        out_shape=tuple(pltpu.HBM(shape, jnp.float32) for shape in outputs),
        in_specs=[vmem] * (len(got) + 3),
        out_specs=(hbm, hbm),
        scratch_shapes=[pltpu.VMEM(shape, jnp.float32) for shape in outputs]
        + [
            pltpu.VMEM((levels, blocks, LANES), jnp.float32),
            pltpu.SemaphoreType.DMA((levels + 1,)),
        ],
        compiler_params=params,
        name="finish",
    )(*got, mean_warmth, limit, basin)
    if dests != lon:
        first = lax.axis_index("lon") * share % SUB
        transport = lax.dynamic_slice_in_dim(transport, first, share, 2)
    return eddy, jnp.transpose(transport, (0, 3, 1, 2))


def solution(mesh):
    return jax.shard_map(
        shards,
        mesh=mesh,
        in_specs=(
            P(None, None, "lat", "lon"),
            P(None, None, "lat", "lon"),
            P("lat", "lon"),
            P("lat", "lon"),
            P("lat", "lon"),
        ),
        out_specs=(P(None, "lat", "lon"), P(None, None, None, ("lat", "lon"))),
        check_vma=False,
    )
```

```python
import functools
import math

import jax
import jax.numpy as jnp
from jax import lax
from jax.experimental import pallas as pl
from jax.experimental.pallas import tpu as pltpu
from jax.sharding import PartitionSpec as P

BASINS = 10
SUB = 8
LANES = 128
CUT = 32
GRANT = 16 * 1024 * 1024


def cover(total, unit):
    return -(-total // unit)


def iota(axis):
    return lax.broadcasted_iota(jnp.int32, (SUB, LANES), axis)


def pick_lanes(tiles, start, width):
    first, shift = divmod(start, LANES)
    if shift == 0:
        return tiles[first]
    left = pltpu.roll(tiles[first], LANES - shift, 1)
    if shift + width <= LANES:
        return left
    right = pltpu.roll(tiles[first + 1], LANES - shift, 1)
    return jnp.where(lax.broadcasted_iota(jnp.int32, left.shape, 1) < LANES - shift, left, right)


def edge_kernel(dims, warmth, flag, floor, edge, rows_buf, flag_buf, floor_buf, sem):
    snapshots, levels = dims[:2]
    first = slice(0, SUB)
    copies = [
        pltpu.make_async_copy(flag.at[first, :], flag_buf, sem.at[snapshots]),
        pltpu.make_async_copy(floor.at[first, :], floor_buf, sem.at[snapshots + 1]),
    ] + [
        pltpu.make_async_copy(warmth.at[t, :, first, :], rows_buf.at[t], sem.at[t])
        for t in range(snapshots)
    ]
    for copy in copies:
        copy.start()
    for copy in copies:
        copy.wait()
    depth = (flag_buf[0:1, :] * floor_buf[0:1, :]).astype(jnp.float32)
    edge[snapshots * levels : snapshots * levels + 1, :] = depth
    for t in range(snapshots):
        for k in range(levels):
            edge[t * levels + k : t * levels + k + 1, :] = rows_buf[t, k, 0:1, :]


def prepare(dims, rows_of, room):
    snapshots, levels = dims[:2]
    get_v, get_w, put_mean = rows_of
    for k in range(levels):
        v = [get_v(t, k) for t in range(snapshots)]
        w = [get_w(t, k) for t in range(snapshots)]
        mv = sum(v[1:], v[0]) * (1.0 / snapshots)
        mw = sum(w[1:], w[0]) * (1.0 / snapshots)
        cross = sum((a - mv) * (b - mw) for a, b in zip(v, w)) * (1.0 / snapshots)
        put_mean(k, mw)
        for at, value in enumerate(w + [mv * mw, cross, mw]):
            room[k, at] = value


def multiply(dims, group, get_v, room, shallow, label):
    snapshots = dims[0]
    width = BASINS * SUB
    nothing = jnp.zeros((SUB, LANES), jnp.float32)

    def level_data(k):
        v = [get_v(t, k) for t in range(snapshots)]
        rest = [room[k, at] for at in range(snapshots + 3)]
        return jnp.concatenate(v + rest + [jnp.ones((SUB, LANES), jnp.float32)], axis=0)

    def level_hot(k):
        masked = jnp.where(shallow > float(k), label, -1)
        return [jnp.where(masked == b, 1.0, 0.0) for b in range(BASINS)]

    data = jnp.concatenate([level_data(k) for k in group], axis=1)
    columns = []
    for k in group:
        column = [nothing] * (group[0] * width % LANES // SUB)
        for other in group:
            column += level_hot(k) if other == k else [nothing] * BASINS
        columns.append(jnp.concatenate(column, axis=0))
    hot = jnp.concatenate(columns, axis=1).astype(jnp.bfloat16)
    exact, height = 2 * snapshots * SUB, data.shape[0]
    cuts = list(range(0, exact, CUT)) + [exact, height]
    parts, spans = [], []
    for at, end in zip(cuts, cuts[1:]):
        rest = data[at:end]
        count = 2 if at < exact else 3
        for piece in range(count):
            parts.append(rest.astype(jnp.bfloat16))
            if piece < count - 1:
                rest = rest - parts[-1].astype(jnp.float32)
        spans.append((end - at, count))
    dots = lax.dot_general(
        jnp.concatenate(parts, axis=0),
        hot,
        (((1,), (1,)), ((), ())),
        preferred_element_type=jnp.float32,
    )
    sums, at = [], 0
    for size, count in spans:
        x = dots[at : at + size]
        for piece in range(1, count):
            x = x + dots[at + piece * size : at + (piece + 1) * size]
        sums.append(x)
        at += size * count
    total = jnp.concatenate(sums, axis=0)
    spare = -total.shape[1] % LANES
    if spare:
        total = jnp.concatenate([total, jnp.zeros((total.shape[0], spare), jnp.float32)], axis=1)
    return total


def extract(dims, group, total, done):
    quantities = 2 * dims[0] + 4
    sub, lane = iota(0), iota(1)
    diagonal = lane % SUB
    tile, shift = divmod(group[0] * BASINS * SUB, LANES)
    for c in range(total.shape[1] // LANES):
        groups = []
        for g in range(quantities // SUB):
            acc = None
            for s in range(SUB):
                q = g * SUB + s
                row = jnp.take_along_axis(
                    total[q * SUB : (q + 1) * SUB, c * LANES : (c + 1) * LANES],
                    diagonal,
                    axis=0,
                    mode="promise_in_bounds",
                )
                acc = row if acc is None else jnp.where(sub == s, row, acc)
            if done[tile + c] is not None:
                acc = jnp.where(lane < shift, done[tile + c][g * SUB : (g + 1) * SUB], acc)
            groups.append(acc)
        done[tile + c] = jnp.concatenate(groups, axis=0)


def level_groups(dims):
    return [tuple(range(k, min(k + 2, dims[1]))) for k in range(0, dims[1], 2)]


def store_block(dims, n, done, keep, give):
    quantities = 2 * dims[0] + 4
    put_own, put_shared = writers(dims, n, keep, give)
    for c in range(dims[4]):
        put_own(c, done[c])
        for q in range(2):
            put_shared(c * 2 + q, done[c][quantities - 2 + q : quantities - 1 + q])


def writers(dims, n, keep, give):
    snapshots, levels, rows, blocks, tiles, dests, per_dest = dims
    quantities = 2 * snapshots + 4
    own_rows = tiles * quantities
    dest, inner = (n // per_dest, n % per_dest) if per_dest > 1 else (n, 0)
    halves = (keep,) if give is None else (keep, give)
    half = dest if give is None else dest // 2
    shared_at = keep.shape[0] - 2 * tiles * blocks

    def put_own(c, value):
        base = (half * per_dest + inner) * own_rows + c * quantities
        if not isinstance(base, int):
            base = pl.multiple_of(base, SUB)
        at = pl.ds(base, quantities)
        if give is None:
            keep[at, :] = value
            return
        me = lax.axis_index("lon")
        mine = (me % 2 == dest % 2) == (me // 2 == dest // 2)

        @pl.when(mine)
        def _():
            keep[at, :] = value

        @pl.when(jnp.logical_not(mine))
        def _():
            give[at, :] = value

    def put_shared(place, value):
        for ref in halves:
            ref[pl.ds(shared_at + place * blocks + n, 1), :] = value

    return put_own, put_shared


def inner_kernel(dims, pairs, flow, warmth, flag, floor, basin, *refs):
    blocks, tiles = dims[3:5]
    outs, room = refs[:-1], refs[-1]
    keep, give = outs[:2] if pairs else (outs[0], None)
    mean_warmth, limit = outs[-2:]

    def span(n):
        at = n * SUB if isinstance(n, int) else pl.multiple_of(n * SUB, SUB)
        return pl.ds(at, SUB), pl.ds(at + 1, SUB)

    def rows_of(n):
        here, north = span(n)

        def put_mean(k, value):
            mean_warmth[k, here, :] = value

        def get_v(t, k):
            return flow[t, k, here, :]

        def get_w(t, k):
            return 0.5 * (warmth[t, k, here, :] + warmth[t, k, north, :])

        return get_v, get_w, put_mean

    def several(ns):
        work = []
        for n in ns:
            here, north = span(n)
            depth = (flag[here, :] * floor[here, :]).astype(jnp.float32)
            upper = (flag[north, :] * floor[north, :]).astype(jnp.float32)
            shallow = jnp.minimum(depth, upper)
            limit[here, :] = shallow
            work.append((n, rows_of(n), shallow, basin[here, :], [None] * tiles))
        totals = []
        rooms = [room.at[i] for i in range(7)]
        for (n, rows, shallow, label, done), r in zip(work, rooms):
            prepare(dims, rows, r)
        for group in level_groups(dims):
            for (n, rows, shallow, label, done), r in zip(work, rooms):
                totals.append((group, done, multiply(dims, group, rows[0], r, shallow, label)))
        for group, done, total in totals:
            extract(dims, group, total, done)

        for n, _, _, _, done in work:
            store_block(dims, n, done, keep, give)

    def body(i, carry):
        several([i * 7 + j for j in range(7)])
        return carry

    lax.fori_loop(0, (blocks - 1) // 7, body, 0)
    rest = (blocks - 1) % 7
    if rest:
        several(list(range(blocks - 1 - rest, blocks - 1)))


def last_kernel(dims, pairs, odd_halo, even_halo, flow, warmth, flag, floor, basin, *refs):
    snapshots, levels, rows, blocks = dims[:4]
    refs, room = refs[:-1], refs[-1]
    outs = refs[len(refs) // 2 :]
    keep, give = outs[:2] if pairs else (outs[0], None)
    mean_warmth, limit = outs[-2:]
    here = slice(rows - SUB, rows)
    below = lax.broadcasted_iota(jnp.int32, (SUB, LANES), 0) < SUB - 1

    lat = lax.axis_index("lat")
    even = lat % 2 == 0
    inside = jnp.where(lat < lax.axis_size("lat") - 1, 1.0, 0.0)

    def north(block, n):
        row = jnp.where(even, even_halo[n : n + 1, :], odd_halo[n : n + 1, :]) * inside
        return jnp.where(below, pltpu.roll(block, SUB - 1, 0), row)

    depth = (flag[here, :] * floor[here, :]).astype(jnp.float32)
    edge_at = snapshots * levels
    shallow = jnp.minimum(depth, north(depth, edge_at))
    limit[here, :] = shallow

    def put_mean(k, value):
        mean_warmth[k, here, :] = value

    def get_v(t, k):
        return flow[t, k, here, :]

    def get_w(t, k):
        block = warmth[t, k, here, :]
        return 0.5 * (block + north(block, t * levels + k))

    room = room.at[0]
    prepare(dims, (get_v, get_w, put_mean), room)
    done = [None] * dims[4]
    totals = [
        multiply(dims, group, get_v, room, shallow, basin[here, :]) for group in level_groups(dims)
    ]
    for group, total in zip(level_groups(dims), totals):
        extract(dims, group, total, done)
    store_block(dims, blocks - 1, done, keep, give)


def spare_lanes(dims):
    snapshots, levels, rows, blocks, tiles, dests, per_dest = dims
    quantities = 2 * snapshots + 4
    used = levels * BASINS * SUB - (tiles - 1) * LANES
    fits = 2 * used <= LANES and 2 * blocks <= quantities - 4 and blocks % SUB == 0
    return fits, used, (tiles - 1) * quantities


def pair_kernel(dims, keep, came, *outs):
    tiles, per_dest = dims[4], dims[6]
    own_rows = per_dest * tiles * (2 * dims[0] + 4)
    chips = len(outs)
    shared = chips * own_rows
    chip = lax.axis_index("lon") // 2
    common = keep[shared:, :] + came[shared:, :]
    fits, used, start = spare_lanes(dims)
    for offset, out in enumerate(outs):
        at = pl.multiple_of((chip ^ offset) * own_rows, SUB)
        own = keep[pl.ds(at, own_rows), :] + came[pl.ds(at, own_rows), :]
        out[0:own_rows, :] = own
        if fits:
            rest = out.shape[0] - own_rows
            size = common.shape[0] - rest
            moved = pltpu.roll(common[rest:], used, 1)
            lane = lax.broadcasted_iota(jnp.int32, moved.shape, 1)
            out[start : start + size, :] = jnp.where(lane < used, own[start : start + size], moved)
            out[own_rows:, :] = common[:rest]
        else:
            out[own_rows:, :] = common


def finish_kernel(dims, scaling, packed, *refs):
    mean_warmth, limit, basin, eddy_out, transport_out, eddy, transport, flat, sem = refs[-9:]
    snapshots, levels, rows, blocks, tiles, dests, per_dest = dims
    width = BASINS * SUB
    quantities = 2 * snapshots + 4
    own_rows = tiles * quantities
    sub, lane = iota(0), iota(1)
    got = refs[:-9]
    if len(got[0].shape) == 3:
        got = [got[0].at[d] for d in range(got[0].shape[0])]
    mine = got[0][...]
    for part in got[1:]:
        mine = mine + part[...]
    shared = mine[per_dest * own_rows :]
    if packed:
        _, used, start = spare_lanes(dims)
        beside = mine[start : start + 2 * blocks]
        shared = jnp.concatenate([shared, pltpu.roll(beside, LANES - used, 1)], axis=0)
    bar = []
    for c in range(tiles):
        at = c * 2 * blocks
        bar.append(shared[at : at + blocks] / jnp.maximum(shared[at + blocks : at + 2 * blocks], 1.0))
    for k in range(levels):
        flat[k] = pick_lanes(bar, k * width, width)
    copies = []
    for k in range(levels):
        for n in range(blocks):
            where = basin[n * SUB : (n + 1) * SUB, :] * SUB + sub
            row = jnp.broadcast_to(flat[k, n : n + 1, :], (SUB, LANES))
            cell = jnp.take_along_axis(row, where, axis=1, mode="promise_in_bounds")
            deep = limit[n * SUB : (n + 1) * SUB, :] > float(k)
            star = mean_warmth[k, n * SUB : (n + 1) * SUB, :] - cell
            eddy[k, n * SUB : (n + 1) * SUB, :] = jnp.where(deep, star, 0.0)
        copies.append(pltpu.make_async_copy(eddy.at[k], eddy_out.at[k], sem.at[k]))
        copies[-1].start()
    spread = jnp.minimum(lane, BASINS - 1) * SUB + sub
    for i in range(per_dest):
        terms = []
        for c in range(tiles):
            own = mine[i * own_rows + c * quantities : i * own_rows + (c + 1) * quantities]
            count = own[quantities - 1 : quantities]
            floor = jnp.maximum(count, 1.0)
            v = own[:snapshots] / floor
            w = own[snapshots : 2 * snapshots] / floor
            bar_v = jnp.sum(v, axis=0, keepdims=True) * (1.0 / snapshots)
            bar_w = jnp.sum(w, axis=0, keepdims=True) * (1.0 / snapshots)
            swing = jnp.sum((v - bar_v) * (w - bar_w), axis=0, keepdims=True) * (1.0 / snapshots)
            mean_part = count * bar_v * bar_w
            swing = count * swing
            product = own[2 * snapshots : 2 * snapshots + 1]
            cross = own[2 * snapshots + 1 : 2 * snapshots + 2]
            four = [mean_part, product - mean_part, swing, cross - swing]
            terms.append(scaling * jnp.concatenate(four + four, axis=0))
        for k in range(levels):
            level = pick_lanes(terms, k * width, width)
            for term in range(4):
                row = jnp.broadcast_to(level[term : term + 1], (SUB, LANES))
                cell = jnp.take_along_axis(row, spread, axis=1, mode="promise_in_bounds")
                transport[term, k, i * SUB : (i + 1) * SUB, :] = cell[:, :BASINS]
    copies.append(pltpu.make_async_copy(transport, transport_out, sem.at[levels]))
    copies[-1].start()
    for copy in copies:
        copy.wait()


def neighbours(lat, lon, first):
    route = []
    for i in range(lat):
        other = i + 1 if (i - first) % 2 == 0 else i - 1
        for j in range(lon):
            across = j ^ 1 if lon % 2 == 0 else j
            if not 0 <= other < lat:
                target = i * lon + across
            elif other < i:
                target = other * lon + j
            else:
                target = other * lon + (across if i > 0 else j)
            route.append((i * lon + j, target))
    return route


def shards(flow, warmth, flag, floor, basin):
    snapshots, levels, rows, cols = flow.shape
    lon, lat = lax.axis_size("lon"), lax.axis_size("lat")
    scaling = 1.0 / math.sqrt(cols * lon)
    share = rows // lon
    blocks = rows // SUB
    per_dest = max(1, share // SUB)
    dests = blocks // per_dest
    width = BASINS * SUB
    tiles = cover(levels * width, LANES)
    quantities = 2 * snapshots + 4
    dims = (snapshots, levels, rows, blocks, tiles, dests, per_dest)
    own_rows, shared_rows = per_dest * tiles * quantities, tiles * 2 * blocks
    pairs = dests == lon and lon in (2, 4, 8)

    vmem = pl.BlockSpec(memory_space=pltpu.VMEM)
    hbm = pl.BlockSpec(memory_space=pl.ANY)
    params = pltpu.CompilerParams(vmem_limit_bytes=GRANT)

    def near(x):
        return pltpu.with_memory_space_constraint(x, pltpu.VMEM)

    def far(x):
        return pltpu.with_memory_space_constraint(x, pltpu.HBM)

    edge = pl.pallas_call(
        functools.partial(edge_kernel, dims),
        out_shape=pltpu.VMEM((snapshots * levels + 1, cols), jnp.float32),
        in_specs=[hbm] * 3,
        out_specs=vmem,
        scratch_shapes=[
            pltpu.VMEM((snapshots, levels, SUB, cols), jnp.float32),
            pltpu.VMEM((SUB, cols), jnp.int32),
            pltpu.VMEM((SUB, cols), jnp.int32),
            pltpu.SemaphoreType.DMA((snapshots + 2,)),
        ],
        compiler_params=params,
        cost_estimate=pl.CostEstimate(flops=10000000000, bytes_accessed=8 << 20, transcendentals=0),
        name="edge",
    )(far(warmth), far(flag), far(floor))
    halos = tuple(
        lax.ppermute(edge, ("lat", "lon"), neighbours(lat, lon, first)) for first in range(2)
    )

    flow, warmth, flag, floor, basin = (near(x) for x in (flow, warmth, flag, floor, basin))
    half = pltpu.VMEM((dests // 2 * own_rows + shared_rows, LANES), jnp.float32)
    full = pltpu.VMEM((dests * own_rows + shared_rows, LANES), jnp.float32)
    results = ((half, half) if pairs else (full,)) + (
        pltpu.VMEM((levels, rows, cols), jnp.float32),
        pltpu.VMEM((rows, cols), jnp.float32),
    )
    room = pltpu.VMEM((7, levels, snapshots + 3, SUB, cols), jnp.float32)
    sums = pl.pallas_call(
        functools.partial(inner_kernel, dims, pairs),
        out_shape=results,
        in_specs=[vmem] * 5,
        out_specs=(vmem,) * len(results),
        scratch_shapes=[room],
        compiler_params=params,
        name="inner_rows",
    )(flow, warmth, flag, floor, basin)
    sums = pl.pallas_call(
        functools.partial(last_kernel, dims, pairs),
        out_shape=results,
        in_specs=[vmem] * (7 + len(results)),
        out_specs=(vmem,) * len(results),
        input_output_aliases={7 + i: i for i in range(len(results))},
        scratch_shapes=[room],
        compiler_params=params,
        name="last_rows",
    )(*halos[::-1], flow, warmth, flag, floor, basin, *sums)
    mean_warmth, limit = sums[-2:]

    if pairs:
        keep, give = sums[:2]
        came = lax.ppermute(give, "lon", [(i, i ^ 1) for i in range(lon)])
        beside = 2 * blocks if spare_lanes(dims)[0] else 0
        message = pltpu.VMEM((own_rows + shared_rows - beside, LANES), jnp.float32)
        chips = lon // 2
        messages = pl.pallas_call(
            functools.partial(pair_kernel, dims),
            out_shape=(message,) * chips,
            in_specs=[vmem, vmem],
            out_specs=(vmem,) * chips,
            compiler_params=params,
            name="pair_sums",
        )(keep, came)
        far_first = list(reversed(range(1, chips)))
        order = far_first[1:2] + far_first[:1] + far_first[2:]
        got = messages[:1] + tuple(
            lax.ppermute(messages[m], "lon", [(i, i ^ (2 * m + 1)) for i in range(lon)])
            for m in order
        )
    else:
        own, shared = sums[0][: dests * own_rows], sums[0][dests * own_rows :]
        sent = jnp.concatenate(
            [own.reshape(dests, own_rows, LANES), jnp.broadcast_to(shared, (dests, shared_rows, LANES))],
            axis=1,
        )
        if dests != lon:
            sent = jnp.repeat(sent, lon // dests, axis=0, total_repeat_length=lon)
        got = (lax.all_to_all(sent, "lon", 0, 0),)

    outputs = ((levels, rows, cols), (4, levels, per_dest * SUB, BASINS))
    eddy, transport = pl.pallas_call(
        functools.partial(finish_kernel, dims, scaling, pairs and spare_lanes(dims)[0]),
        out_shape=tuple(pltpu.HBM(shape, jnp.float32) for shape in outputs),
        in_specs=[vmem] * (len(got) + 3),
        out_specs=(hbm, hbm),
        scratch_shapes=[pltpu.VMEM(shape, jnp.float32) for shape in outputs]
        + [
            pltpu.VMEM((levels, blocks, LANES), jnp.float32),
            pltpu.SemaphoreType.DMA((levels + 1,)),
        ],
        compiler_params=params,
        name="finish",
    )(*got, mean_warmth, limit, basin)
    if dests != lon:
        first = lax.axis_index("lon") * share % SUB
        transport = lax.dynamic_slice_in_dim(transport, first, share, 2)
    return eddy, jnp.transpose(transport, (0, 3, 1, 2))


def solution(mesh):
    return jax.shard_map(
        shards,
        mesh=mesh,
        in_specs=(
            P(None, None, "lat", "lon"),
            P(None, None, "lat", "lon"),
            P("lat", "lon"),
            P("lat", "lon"),
            P("lat", "lon"),
        ),
        out_specs=(P(None, "lat", "lon"), P(None, None, None, ("lat", "lon"))),
        check_vma=False,
    )
```
